128 devices in a mesh: seq: 8 (over x, y_hi), fsdp: 16 (over z, y_lo, core).
Axes of the slice: x: 4, y: 4 (y_hi: 2, y_lo: 2; y = y_hi * 2 + y_lo), z: 4, core: 2. Of those that a mesh axis runs over, the one named last changes fastest.
Arguments:
- tokens: bfloat16 [16, 1024, 8192], P('fsdp', 'seq'), may hold values from -6 to 6
- norm_gain: float32 [8192], replicated, may hold values from 0.3 to 3
- w_query: bfloat16 [8192, 4096], P(('seq', 'fsdp')), may hold values from -1 to 1
- key_weight: bfloat16 [8192, 512], P(('seq', 'fsdp')), may hold values from -1 to 1
- value_weight: bfloat16 [8192, 512], P(('seq', 'fsdp')), may hold values from -0.0625 to 0.0625
- w_out: bfloat16 [4096, 8192], P(None, ('seq', 'fsdp')), may hold values from -0.09375 to 0.09375
Outputs:
- result: float32 [16, 1024, 8192], P('fsdp', 'seq')
The draws below stay inside these ranges and needn't reach their ends.
All inputs are finite; a program needn't handle non-finite values.
Results may differ from the reference program's by a relative error of at most 0.04.
Values may be sent and summed in bfloat16 or wider, within the bound.
A program may use at most 128 MiB of HBM per device.

```python
import math
import jax
import jax.numpy as jnp
from jax import lax

MODEL_WIDTH = 8192
HQ = 32
KEY_VALUE_HEADS = 4
HEAD_SIZE = 128
GROUP = 8
SEQUENCE_TOKENS = 1024
SEQS = 16
N_SEQ = 8


def projection_sample(key, head_count):
    normal_draw = jax.random.normal(jax.random.fold_in(key, 11), (MODEL_WIDTH, head_count * HEAD_SIZE), jnp.float32)
    normal_draw = jnp.clip(normal_draw, -6.0, 6.0) / math.sqrt(MODEL_WIDTH)
    normal_draw = jnp.clip(normal_draw, -1.0, 1.0)
    return normal_draw.astype(jnp.bfloat16)


def draw_w_query(key, part):
    return projection_sample(jax.random.fold_in(key, 101), HQ)


def draw_key_weight(key, part):
    return projection_sample(jax.random.fold_in(key, 202), KEY_VALUE_HEADS)


def shard_levels(rng, extent, split, smallest, top_value):
    def one(position, parts):
        heights = jax.random.uniform(jax.random.fold_in(jax.random.fold_in(rng, 6), position), (parts,), jnp.float32, smallest / len(split), top_value / len(split))
        return jnp.repeat(jnp.exp(heights), extent[position] // parts).reshape((-1,) + (1,) * (len(extent) - position - 1))

    level = one(*split[0])
    for cut in split[1:]:
        level = level * one(*cut)
    return level


def bell_draw(own_key, extent, deviation, bound, shards=(), kind=jnp.bfloat16):
    entries = jax.random.normal(own_key, extent, jnp.float32) * deviation
    if len(shards) > 0:
        entries = shard_levels(own_key, extent, shards, -0.22, 0.18) * entries
    return jnp.clip(entries, min=-bound, max=bound).astype(kind)


def setup_inputs(seed: int = 0) -> dict:
    splits = jax.random.split(jax.random.key(seed), 7)
    tokens = bell_draw(splits[0], (SEQS, SEQUENCE_TOKENS, MODEL_WIDTH), 1.0, 6.0, ((0, 16), (1, 8)))
    norm_gain = jnp.clip(jnp.exp(jax.random.uniform(splits[1], (MODEL_WIDTH,), jnp.float32, math.log(0.3), math.log(3.0))), 0.3, 3.0)
    w_query = draw_w_query(jax.random.fold_in(splits[6], 71), 0)
    key_weight = draw_key_weight(jax.random.fold_in(splits[6], 71), 0)
    value_weight = bell_draw(splits[4], (MODEL_WIDTH, KEY_VALUE_HEADS * HEAD_SIZE), MODEL_WIDTH ** -0.5, 0.0625, ((0, 128),))
    w_out = bell_draw(splits[5], (HQ * HEAD_SIZE, MODEL_WIDTH), (HQ * HEAD_SIZE) ** -0.5, 0.09375, ((1, 128),))
    return {"tokens": tokens, "norm_gain": norm_gain, "w_query": w_query, "key_weight": key_weight, "value_weight": value_weight, "w_out": w_out}


def rms_norm(sequence_rows, norm_gain):
    floats = sequence_rows.astype(jnp.float32)
    mean_square = lax.optimization_barrier(jnp.mean(floats * floats, axis=-1, keepdims=True))
    return (floats * lax.rsqrt(mean_square + 1e-05) * norm_gain).astype(jnp.bfloat16)

def apply_projection(normed_input, weight):
    block = MODEL_WIDTH // N_SEQ
    running = jnp.zeros((normed_input.shape[0], weight.shape[1]), jnp.float32)
    for block_index in range(N_SEQ):
        partial_sum = jnp.dot(normed_input[:, block_index * block:(block_index + 1) * block], weight[block_index * block:(block_index + 1) * block], preferred_element_type=jnp.float32)
        rounded = lax.optimization_barrier(partial_sum.astype(jnp.bfloat16))
        running = running + rounded.astype(jnp.float32)
    return running.astype(jnp.bfloat16)

def reference(tokens, norm_gain, w_query, key_weight, value_weight, w_out):
    scale = HEAD_SIZE ** (-0.5)
    row_ids = lax.broadcasted_iota(jnp.int32, (SEQUENCE_TOKENS, SEQUENCE_TOKENS), 0)
    col_ids = lax.broadcasted_iota(jnp.int32, (SEQUENCE_TOKENS, SEQUENCE_TOKENS), 1)
    causal = row_ids >= col_ids

    def one_sequence(sequence_rows):
        normed_input = rms_norm(sequence_rows, norm_gain)
        queries = apply_projection(normed_input, w_query).reshape(SEQUENCE_TOKENS, HQ, HEAD_SIZE)
        key_tensor = apply_projection(normed_input, key_weight).reshape(SEQUENCE_TOKENS, KEY_VALUE_HEADS, HEAD_SIZE)
        value_tensor = apply_projection(normed_input, value_weight).reshape(SEQUENCE_TOKENS, KEY_VALUE_HEADS, HEAD_SIZE)

        def one_head(head_index):
            query_head = lax.dynamic_index_in_dim(queries, head_index, 1, keepdims=False)
            kv_index = head_index // GROUP
            key_head = lax.dynamic_index_in_dim(key_tensor, kv_index, 1, keepdims=False)
            value_head = lax.dynamic_index_in_dim(value_tensor, kv_index, 1, keepdims=False)
            scores = jnp.dot(query_head, key_head.T, preferred_element_type=jnp.float32) * scale
            scores = jnp.where(causal, scores, jnp.float32(-1e+30))
            top = lax.optimization_barrier(jnp.max(scores, axis=-1, keepdims=True))
            weights = jnp.exp(scores - top)
            probs = (weights / lax.optimization_barrier(jnp.sum(weights, axis=-1, keepdims=True))).astype(jnp.bfloat16)
            return jnp.dot(probs, value_head, preferred_element_type=jnp.float32).astype(jnp.bfloat16)
        heads = lax.map(one_head, jnp.arange(HQ, dtype=jnp.int32))
        heads = jnp.transpose(heads, (1, 0, 2)).reshape(SEQUENCE_TOKENS, HQ * HEAD_SIZE)
        branch = jnp.dot(heads, w_out, preferred_element_type=jnp.float32).astype(jnp.bfloat16)
        return sequence_rows.astype(jnp.float32) + branch.astype(jnp.float32)
    return lax.map(one_sequence, tokens)
```

```python
import jax
import jax.numpy as jnp
from jax import lax
from jax.experimental import pallas as pl
from jax.experimental.pallas import tpu as pltpu
from jax.sharding import PartitionSpec as P

HD = 128
BLK = 128
D = 8192
NQ = 1024
NKV = 256
NW = NQ + NKV
NO = 2048
MESH = pl.DeviceIdType.MESH
SLOT = (0, 1, 3, 2)


def kernel(
    tok, gain, wq, wk, wv, wot, out,
    W, WO, X, Q, KV, HG, OB, acc,
    loc, xs, xr, xss, xrs, wS, wR, wRD, oS, oR, oRD, kvs, kvr, hs, hr, os_, or_, ol,
):
    sx = lax.axis_index("seq")
    f = lax.axis_index("fsdp")
    x, yh = sx // 2, sx % 2
    z, yl, c = f // 4, (f // 2) % 2, f % 2
    y = 2 * yh + yl
    p = yh * 16 + f

    def dev(xx, yy, zz, cc):
        return (2 * xx + yy // 2, 4 * zz + 2 * (yy % 2) + cc)

    def at_x(r):
        return dev((x + r) % 4, y, z, c)

    sib = dev(x, y, z, 1 - c)
    pair = dev(x, (y + 2) % 4, z, c)

    barrier = pltpu.get_barrier_semaphore()
    peers = [at_x(1), at_x(2), at_x(3), sib, pair]
    peers += [dev(x, (y + 1) % 4, z, c), dev(x, (y + 3) % 4, z, c)]
    peers += [dev(x, y, (z + 1) % 4, c), dev(x, y, (z + 3) % 4, c)]
    for d in peers:
        pl.semaphore_signal(barrier, inc=1, device_id=d, device_id_type=MESH)

    def own_parts(xx, row):
        cq = pl.ds(pl.multiple_of(xx * NQ, NQ), NQ)
        ck = pl.ds(pl.multiple_of(xx * HD, HD), HD)
        return (
            (wq.at[:, cq], W.at[row, p, :, 0:NQ]),
            (wk.at[:, ck], W.at[row, p, :, NQ : NQ + HD]),
            (wv.at[:, ck], W.at[row, p, :, NQ + HD : NW]),
        )

    tok_in = pltpu.make_async_copy(tok, X.at[0], loc.at[0])
    tok_in.start()
    wo_in = pltpu.make_async_copy(wot, WO.at[p], loc.at[1])
    wo_in.start()
    w_in = [
        pltpu.make_async_copy(s, d, loc.at[2 + k])
        for k, (s, d) in enumerate(own_parts(x, x))
    ]
    for cp in w_in:
        cp.start()

    pl.semaphore_wait(barrier, len(peers))

    xsends = []
    for r in (1, 3, 2):
        for k, (s, d) in enumerate(own_parts((x + r) % 4, x)):
            cp = pltpu.make_async_remote_copy(
                s, d, xs.at[r, k], xr.at[4 - r, k], device_id=at_x(r), device_id_type=MESH
            )
            cp.start()
            xsends.append(cp)

    def gather(buf, S, R, RD, is_w):
        def piece(h, pp):
            return buf.at[h, pp] if is_w else buf.at[pp, h]

        def coords(h, a1, a2):
            g, sg = h // 2, 1 - 2 * (h % 2)
            yy = (y + 4 + sg * (a1 * g + a2 * (1 - g))) % 4
            zz = (z + 4 + sg * (a1 * (1 - g) + a2 * g)) % 4
            return yy, zz

        def ref(h, u1, u2):
            yy, zz = coords(h, u1, u2)
            return piece(h, (yy // 2) * 16 + 4 * zz + 2 * (yy % 2) + c)

        def send(h, u1, u2, k):
            a1, a2 = ((1, 0), (-1, 0), (0, 1), (0, -1))[k]
            yy, zz = coords(h, a1, a2)
            r = ref(h, u1, u2)
            pltpu.make_async_remote_copy(
                r, r, S.at[k], R.at[h, (u1 - a1) % 4, (u2 - a2) % 4],
                device_id=dev(x, yy, zz, c), device_id_type=MESH,
            ).start()

        def across(h, u1, u2):
            r = ref(h, u1, u2)
            pltpu.make_async_remote_copy(
                r, r, S.at[4], RD, device_id=sib, device_id_type=MESH
            ).start()

        def recv(h, u1, u2):
            r = ref(h, u1, u2)
            pltpu.make_async_remote_copy(
                r, r, S.at[4], R.at[h, u1, u2], device_id=sib, device_id_type=MESH
            ).wait_recv()

        def over_pieces(steps):
            def one(h, _):
                for u1, u2, ks in steps:
                    if (u1, u2) != (0, 0):
                        recv(h, u1, u2)
                    for k in ks:
                        send(h, u1, u2, k)
                    across(h, u1, u2)
                return 0

            lax.fori_loop(0, 4, one, 0)

        def many(n):
            return buf.at[:, 0 : n // 4] if is_w else buf.at[0 : n // 4]

        def whole(sem, n):
            return pltpu.make_async_remote_copy(
                many(n), many(n), sem, sem, device_id=sib, device_id_type=MESH
            )

        def wave(n):
            if n == 0:
                over_pieces([(0, 0, (0, 1, 2, 3))])
            elif n == 1:
                over_pieces([(3, 0, (0, 2, 3)), (1, 0, (2, 3))])
            elif n == 2:
                over_pieces([(2, 0, (2, 3)), (0, 3, (2,))])
            elif n == 3:
                over_pieces([(3, 3, (2,)), (1, 3, (2,))])
            elif n == 4:
                over_pieces([(2, 3, (2,)), (0, 1, ()), (0, 2, ())])
            elif n == 5:
                over_pieces([(u, v, ()) for u in (3, 1, 2) for v in (1, 2)])

        def arrived():
            whole(RD, 64).wait_recv()

        def sent():
            for k, n in enumerate((8, 4, 32, 16, 64)):
                whole(S.at[k], n).wait_send()

        return wave, arrived, sent

    w_wave, w_arrived, w_sent = gather(W, wS, wR, wRD, True)
    o_wave, o_arrived, o_sent = gather(WO, oS, oR, oRD, False)

    tok_in.wait()

    def norm(r, _):
        rows = pl.ds(pl.multiple_of(r * 16, 16), 16)
        v = X[0, rows, :].astype(jnp.float32)
        ms = jnp.mean(v * v, axis=-1, keepdims=True)
        X[0, rows, :] = (v * lax.rsqrt(ms + 1e-05) * gain[...]).astype(jnp.bfloat16)
        return 0

    lax.fori_loop(0, BLK // 16, norm, 0)

    def x_piece(a, u, k, start):
        sg = 1 - 2 * a
        r = sg if k == 0 else -sg
        src = X.at[SLOT[(sg * u) % 4], 64 * a : 64 * a + 64]
        dst = X.at[SLOT[(sg * u - r) % 4], 64 * a : 64 * a + 64]
        cp = pltpu.make_async_remote_copy(
            src, dst, xss.at[a, 2 if u else k], xrs.at[a, (u - r * sg) % 4],
            device_id=at_x(r), device_id_type=MESH,
        )
        if start:
            cp.start()
        return cp

    def x_recv(a, u):
        sg = 1 - 2 * a
        d = X.at[SLOT[(sg * u) % 4], 64 * a : 64 * a + 64]
        pltpu.make_async_remote_copy(
            d, d, xss.at[a, 0], xrs.at[a, u], device_id=sib, device_id_type=MESH
        ).wait_recv()

    x_own = [x_piece(a, 0, k, True) for k in (0, 1) for a in (0, 1)]

    wo_in.wait()
    o_wave(0)

    for cp in w_in:
        cp.wait()
    for r in (1, 3, 2):
        for k, (s, d) in enumerate(own_parts((x + r) % 4, (x + r) % 4)):
            pltpu.make_async_remote_copy(
                d, d, xs.at[r, k], xr.at[r, k], device_id=sib, device_id_type=MESH
            ).wait_recv()
    w_wave(0)
    o_wave(1)
    w_wave(1)
    w_wave(2)
    x_fwd = []
    for a in (0, 1):
        x_recv(a, 3)
        x_fwd.append(x_piece(a, 3, 0, True))
    w_wave(3)
    w_wave(4)
    w_wave(5)
    o_wave(2)
    o_wave(3)
    w_arrived()
    for a in (0, 1):
        x_recv(a, 1)

    def project(lo, hi):
        m = (hi - lo) * BLK

        def step(kc, _):
            cols = pl.ds(pl.multiple_of(kc * 1024, 1024), 1024)
            xk = X[lo:hi, :, cols].reshape(m, 1024)
            wkc = W[kc // 2, pl.ds((kc % 2) * 16, 16)].reshape(1024, NW)
            d = jnp.dot(xk, wkc, preferred_element_type=jnp.float32)

            @pl.when(kc == 0)
            def _():
                acc[0:m, :] = d

            @pl.when(kc > 0)
            def _():
                acc[0:m, :] += d

            return 0

        lax.fori_loop(0, 8, step, 0)
        cps = []
        for s in range(lo, hi):
            off = SLOT.index(s)
            i = (x + off) % 4
            rows = slice((s - lo) * BLK, (s - lo + 1) * BLK)
            Q[i] = acc[rows, 0:NQ].astype(jnp.bfloat16)
            KV[2 * i + yh] = acc[rows, NQ:NW].astype(jnp.bfloat16)
            ref = KV.at[2 * i + yh]
            cp = pltpu.make_async_remote_copy(
                ref, ref, kvs.at[off], kvr.at[off], device_id=pair, device_id_type=MESH
            )
            cp.start()
            cps.append(cp)
        return cps

    kv_cps = project(0, 3)
    o_wave(4)
    for a in (0, 1):
        x_recv(a, 2)
    kv_cps += project(3, 4)
    for off in range(4):
        i = (x + off) % 4
        ref = KV.at[2 * i + 1 - yh]
        pltpu.make_async_remote_copy(
            ref, ref, kvs.at[off], kvr.at[off], device_id=pair, device_id_type=MESH
        ).wait_recv()
    o_wave(5)

    scale = HD ** (-0.5)

    def h_ref(j, a, u):
        sg = 1 - 2 * a
        return HG.at[j, (x + 4 + sg * u) % 4, 2 * a : 2 * a + 2]

    def h_send(j, a, u, k):
        sg = 1 - 2 * a
        r = 1 if k != 1 else -1
        ref = h_ref(j, a, u)
        pltpu.make_async_remote_copy(
            ref, ref, hs.at[k], hr.at[j, a, (u - r) % 4],
            device_id=at_x(r * sg), device_id_type=MESH,
        ).start()

    def h_recv(j, a, u):
        ref = h_ref(j, a, u)
        pltpu.make_async_remote_copy(
            ref, ref, hs.at[0], hr.at[j, a, u], device_id=sib, device_id_type=MESH
        ).wait_recv()

    def attend(j, _):
        rows = pl.ds(pl.multiple_of(j * 32, 32), 32)
        for i in range(4):
            nk = (2 * i + 2) * BLK
            q = jnp.concatenate(
                [Q[i, rows, h * HD : (h + 1) * HD] for h in range(8)], axis=0
            )
            kk = KV[0 : 2 * i + 2, :, 0:HD].reshape(nk, HD)
            vv = KV[0 : 2 * i + 2, :, HD:NKV].reshape(nk, HD)
            s = lax.dot_general(
                q, kk, (((1,), (1,)), ((), ())), preferred_element_type=jnp.float32
            ) * scale
            qpos = (2 * i + yh) * BLK + j * 32 + lax.broadcasted_iota(
                jnp.int32, (256, nk), 0
            ) % 32
            kpos = lax.broadcasted_iota(jnp.int32, (256, nk), 1)
            s = jnp.where(qpos >= kpos, s, jnp.float32(-1e30))
            e = jnp.exp(s - jnp.max(s, axis=-1, keepdims=True))
            pr = (e * (1.0 / jnp.sum(e, axis=-1, keepdims=True))).astype(jnp.bfloat16)
            o = jnp.dot(pr, vv, preferred_element_type=jnp.float32).astype(jnp.bfloat16)
            for h in range(8):
                HG[j, x, i, :, h * HD : (h + 1) * HD] = o[h * 32 : (h + 1) * 32]
        for k in (0, 1):
            for a in (0, 1):
                h_send(j, a, 0, k)
        return 0

    lax.fori_loop(0, 4, attend, 0)

    def forward(j, _):
        for a in (0, 1):
            h_recv(j, a, 3)
            h_send(j, a, 3, 2)
        return 0

    lax.fori_loop(0, 4, forward, 0)
    o_arrived()

    def out_ref(j, xx):
        return out.at[
            pl.ds(pl.multiple_of(j * 32, 32), 32), pl.ds(pl.multiple_of(xx * NO, NO), NO)
        ]

    def mix(j, _):
        for a in (0, 1):
            h_recv(j, a, 1)
            h_recv(j, a, 2)

        def tile(n, _):
            t = jnp.zeros((BLK, 512), jnp.float32)
            for s in range(4):
                wo = WO[pl.ds(n * 8, 8), :, :, s * NQ : (s + 1) * NQ].reshape(512, NQ)
                t += lax.dot_general(
                    HG[j, s].reshape(BLK, NQ), wo, (((1,), (1,)), ((), ())),
                    preferred_element_type=jnp.float32,
                )
            OB[j, :, :, pl.ds(pl.multiple_of(n * 512, 512), 512)] = t.astype(
                jnp.bfloat16
            ).reshape(4, 32, 512)
            return 0

        lax.fori_loop(0, 4, tile, 0)
        for r in (2, 1, 3):
            pltpu.make_async_remote_copy(
                OB.at[j, (x + r) % 4], out_ref(j, x), os_.at[r], or_.at[j, 4 - r],
                device_id=at_x(r), device_id_type=MESH,
            ).start()
        pltpu.make_async_copy(OB.at[j, x], out_ref(j, x), ol).start()
        return 0

    lax.fori_loop(0, 4, mix, 0)

    for cp in xsends + x_own + x_fwd + kv_cps:
        cp.wait_send()
    w_sent()
    o_sent()
    for k in range(3):
        pltpu.make_async_remote_copy(
            HG.at[0], HG.at[0], hs.at[k], hs.at[k], device_id=sib, device_id_type=MESH
        ).wait_send()
    for r in (1, 2, 3):
        pltpu.make_async_remote_copy(
            OB.at[0], OB.at[0], os_.at[r], os_.at[r], device_id=sib, device_id_type=MESH
        ).wait_send()
    pltpu.make_async_copy(OB.at[0], OB.at[0], ol).wait()

    def finish(j, _):
        for r in (1, 2, 3):
            d = out_ref(j, (x + r) % 4)
            pltpu.make_async_remote_copy(
                d, d, os_.at[r], or_.at[j, r], device_id=sib, device_id_type=MESH
            ).wait_recv()
        return 0

    lax.fori_loop(0, 4, finish, 0)


def body(tokens, norm_gain, w_query, key_weight, value_weight, w_out):
    hbm = pl.BlockSpec(memory_space=pltpu.HBM)
    vmem = pl.BlockSpec(memory_space=pltpu.VMEM)
    bf = jnp.bfloat16
    dma = pltpu.SemaphoreType.DMA
    wot = w_out.T.reshape(4, 16, 4096)
    branch = pl.pallas_call(
        kernel,
        out_shape=jax.ShapeDtypeStruct((BLK, D), bf),
        in_specs=[hbm, vmem, hbm, hbm, hbm, hbm],
        out_specs=hbm,
        scratch_shapes=[
            pltpu.VMEM((4, 32, 64, NW), bf),
            pltpu.VMEM((32, 4, 16, 4096), bf),
            pltpu.VMEM((4, BLK, D), bf),
            pltpu.VMEM((4, BLK, NQ), bf),
            pltpu.VMEM((8, BLK, NKV), bf),
            pltpu.VMEM((4, 4, 4, 32, NQ), bf),
            pltpu.VMEM((4, 4, 32, NO), bf),
            pltpu.VMEM((3 * BLK, NW), jnp.float32),
            dma((5,)), dma((4, 3)), dma((4, 3)), dma((2, 3)), dma((2, 4)),
            dma((5,)), dma((4, 4, 4)), dma(()),
            dma((5,)), dma((4, 4, 4)), dma(()),
            dma((4,)), dma((4,)), dma((3,)), dma((4, 2, 4)),
            dma((4,)), dma((4, 4)), dma(()),
        ],
        compiler_params=pltpu.CompilerParams(
            collective_id=0, has_side_effects=True, vmem_limit_bytes=67043328
        ),
        name="sublayer",
    )(tokens[0], norm_gain.reshape(1, D), w_query, key_weight, value_weight, wot)
    return tokens.astype(jnp.float32) + branch[None].astype(jnp.float32)


def solution(mesh):
    placed = (
        P("fsdp", "seq", None),
        P(),
        P(("seq", "fsdp"), None),
        P(("seq", "fsdp"), None),
        P(("seq", "fsdp"), None),
        P(None, ("seq", "fsdp")),
    )
    return jax.shard_map(
        body, mesh=mesh, in_specs=placed, out_specs=P("fsdp", "seq", None), check_vma=False
    )
```

```python
import jax
import jax.numpy as jnp
from jax import lax
from jax.experimental import pallas as pl
from jax.experimental.pallas import tpu as pltpu
from jax.sharding import PartitionSpec as P

HD = 128
BLK = 128
D = 8192
NQ = 1024
NKV = 256
NW = NQ + NKV
NO = 2048
MESH = pl.DeviceIdType.MESH
SLOT = (0, 1, 3, 2)
NX = 4


def kernel(
    tok, gain, wq, wk, wv, wot, out,
    W, WO, X, Q, KV, HG, OB, acc,
    T, loc, xs, xr, xss, xrs, wS, wR, wRD, oS, oR, oRD, kvs, kvr, hs, hr, os_, or_, ol,
):
    sx = lax.axis_index("seq")
    f = lax.axis_index("fsdp")
    x, yh = sx // 2, sx % 2
    z, yl, c = f // 4, (f // 2) % 2, f % 2
    y = 2 * yh + yl
    p = yh * 16 + f

    def dev(xx, yy, zz, cc):
        return (2 * xx + yy // 2, 4 * zz + 2 * (yy % 2) + cc)

    def at_x(r):
        return dev((x + r) % 4, y, z, c)

    sib = dev(x, y, z, 1 - c)
    pair = dev(x, (y + 2) % 4, z, c)

    barrier = pltpu.get_barrier_semaphore()
    peers = [at_x(1), at_x(2), at_x(3), sib, pair]
    peers += [dev(x, (y + 1) % 4, z, c), dev(x, (y + 3) % 4, z, c)]
    peers += [dev(x, y, (z + 1) % 4, c), dev(x, y, (z + 3) % 4, c)]
    for d in peers:
        pl.semaphore_signal(barrier, inc=1, device_id=d, device_id_type=MESH)

    def w_parts(xx, h):
        cq = pl.ds(pl.multiple_of(xx * NQ, NQ), NQ)
        ck = pl.ds(pl.multiple_of(xx * HD, HD), HD)
        return [
            (src.at[:, cc], W.at[h, yh, z, yl, c, :, lo:hi])
            for src, cc, lo, hi in (
                (wq, cq, 0, NQ), (wk, ck, NQ, NQ + HD), (wv, ck, NQ + HD, NW)
            )
        ]

    w_in = [
        pltpu.make_async_copy(s, d, loc.at[2 + k])
        for k, (s, d) in enumerate(w_parts(x, 0))
    ]
    for cp in w_in:
        cp.start()
    khalf = pl.ds(pl.multiple_of(c * 2048, 2048), 2048)
    other = pl.ds(pl.multiple_of((1 - c) * 2048, 2048), 2048)
    tok_in = pltpu.make_async_copy(tok, X.at[0], loc.at[0])
    tok_in.start()
    wo_in = pltpu.make_async_copy(wot.at[:, khalf], T.at[c], loc.at[1])
    wo_in.start()

    with jax.named_scope('p01_barrier'):
        pl.semaphore_wait(barrier, len(peers))

    xsends = []
    for r in (1, 3, 2):
        for k, (s, d) in enumerate(w_parts((x + r) % 4, 4 - r)):
            cp = pltpu.make_async_remote_copy(
                s, d, xs.at[r, k], xr.at[4 - r, k], device_id=at_x(r), device_id_type=MESH
            )
            cp.start()
            xsends.append(cp)
    wo_swap = pltpu.make_async_remote_copy(
        wot.at[:, other], T.at[c], loc.at[8], loc.at[9], device_id=sib, device_id_type=MESH
    )
    wo_swap.start()

    def w_got(r):
        for k, (s, d) in enumerate(w_parts(x, r)):
            pltpu.make_async_remote_copy(
                d, d, xs.at[r, k], xr.at[r, k], device_id=sib, device_id_type=MESH
            ).wait_recv()

    def gather(S, R, RD, piece, many):
        def coords(h, a1, a2):
            g, sg = h // 2, 1 - 2 * (h % 2)
            yy = (y + 4 + sg * (a1 * g + a2 * (1 - g))) % 4
            zz = (z + 4 + sg * (a1 * (1 - g) + a2 * g)) % 4
            return yy, zz

        def ref(h, u1, u2):
            yy, zz = coords(h, u1, u2)
            return piece(h, yy, zz)

        def send(h, u1, u2, k):
            a1, a2 = ((1, 0), (-1, 0), (0, 1), (0, -1))[k]
            yy, zz = coords(h, a1, a2)
            r = ref(h, u1, u2)
            pltpu.make_async_remote_copy(
                r, r, S.at[k], R.at[h, (u1 - a1) % 4, (u2 - a2) % 4],
                device_id=dev(x, yy, zz, c), device_id_type=MESH,
            ).start()

        def across(h, u1, u2):
            r = ref(h, u1, u2)
            pltpu.make_async_remote_copy(
                r, r, S.at[4], RD.at[int(u2 in (1, 2))], device_id=sib, device_id_type=MESH
            ).start()

        def recv(h, u1, u2):
            r = ref(h, u1, u2)
            pltpu.make_async_remote_copy(
                r, r, S.at[4], R.at[h, u1, u2], device_id=sib, device_id_type=MESH
            ).wait_recv()

        def over_pieces(steps, first=0, last=4, d2d=True):
            def one(h, _):
                for u1, u2, ks in steps:
                    if (u1, u2) != (0, 0):
                        recv(h, u1, u2)
                    for k in ks:
                        send(h, u1, u2, k)
                    if d2d:
                        across(h, u1, u2)
                return 0

            lax.fori_loop(first, last, one, 0)

        def whole(sem, n):
            return pltpu.make_async_remote_copy(
                many(n), many(n), sem, sem, device_id=sib, device_id_type=MESH
            )

        def wave(n):
            if n == 1:
                over_pieces([(3, 0, (0, 2, 3)), (1, 0, (2, 3))])
            elif n == 2:
                over_pieces([(2, 0, (2, 3)), (0, 3, (2,))])
            elif n == 3:
                over_pieces([(3, 3, (2,)), (1, 3, (2,))])
            elif n == 4:
                over_pieces([(2, 3, (2,))])
            elif n == 5:
                over_pieces([(u, 1, ()) for u in (0, 3, 1, 2)])
            elif n == 6:
                over_pieces([(u, 2, ()) for u in (0, 3, 1, 2)])

        def arrived(k):
            whole(RD.at[k], 32).wait_recv()

        def sent():
            for k, n in enumerate((8, 4, 32, 16, 64)):
                whole(S.at[k], n).wait_send()

        return over_pieces, wave, arrived, sent

    def w_many(n):
        if n == 64:
            return W.at[0:2]
        if n == 32:
            return W.at[0]
        if n == 16:
            return W.at[0, 0]
        return W.at[0, 0, 0 : n // 4]

    def chunk_of(e):
        return e + (e // 2) * (1 - 2 * (e % 2))

    w_over, w_wave, w_arrived, w_sent = gather(
        wS, wR, wRD, lambda e, yy, zz: W.at[chunk_of(e), yy // 2, zz, yy % 2, c], w_many
    )
    o_over, o_wave, o_arrived, o_sent = gather(
        oS, oR, oRD,
        lambda e, yy, zz: WO.at[(yy // 2) * 16 + 4 * zz + 2 * (yy % 2) + c, e],
        lambda n: WO.at[0 : n // 4],
    )

    own = [(0, 0, (0, 1, 2, 3))]
    with jax.named_scope('p02_w0a'):
        for cp in w_in:
            cp.wait()
        w_over(own, 0, 1)

    with jax.named_scope('p02_tok'):
        tok_in.wait()

    def norm(r, _):
        rows = pl.ds(pl.multiple_of(r * 16, 16), 16)
        v = X[0, rows, :].astype(jnp.float32)
        ms = jnp.mean(v * v, axis=-1, keepdims=True)
        X[0, rows, :] = (v * lax.rsqrt(ms + 1e-05) * gain[...]).astype(jnp.bfloat16)
        return 0

    with jax.named_scope('p03_norm'):
        lax.fori_loop(0, BLK // 16, norm, 0)

    def x_ref(a, o, q):
        return X.at[SLOT[o % 4], 64 * a : 64 * a + 64, q * (D // NX) : (q + 1) * (D // NX)]

    def x_piece(a, u, k, q):
        sg = 1 - 2 * a
        r = sg if k == 0 else -sg
        cp = pltpu.make_async_remote_copy(
            x_ref(a, sg * u, q), x_ref(a, sg * u - r, q),
            xss.at[a, 2 if u else k, q], xrs.at[a, (u - r * sg) % 4, q],
            device_id=at_x(r), device_id_type=MESH,
        )
        cp.start()
        return cp

    def x_recv(a, u, q):
        d = x_ref(a, (1 - 2 * a) * u, q)
        pltpu.make_async_remote_copy(
            d, d, xss.at[a, 0, q], xrs.at[a, u, q], device_id=sib, device_id_type=MESH
        ).wait_recv()

    def x_forward(a, q):
        x_recv(a, 3, q)
        return x_piece(a, 3, 0, q)

    x_own = [x_piece(a, 0, k, q) for k in (0, 1) for q in range(NX) for a in (0, 1)]

    with jax.named_scope('p04_swap'):
        wo_in.wait()
        wo_swap.wait_recv()
        t = T[...].reshape(BLK, 2048)
        for h in range(4):
            WO[p, h] = t[:, 512 * h : 512 * (h + 1)].T

    with jax.named_scope('p05_o0'):
        o_over(own, 0, 2)
    with jax.named_scope('p06_wx1'):
        w_got(1)
        w_got(3)
        w_over([(0, 0, (0, 1))], 1, 3)
        w_over([(0, 0, (2, 3))], 1, 3, False)
    with jax.named_scope('p07_wx2'):
        w_got(2)
        w_over(own, 3, 4)
    with jax.named_scope('p08_w1'):
        w_wave(1)
    with jax.named_scope('p09_w2'):
        w_wave(2)
    with jax.named_scope('p10_xf'):
        x_fwd = [x_forward(a, q) for q in range(NX) for a in (0, 1)]
    with jax.named_scope('p11_w3'):
        w_wave(3)
    with jax.named_scope('p12_w4'):
        w_wave(4)
    with jax.named_scope('p13_o1'):
        o_over(own, 2, 4)
    with jax.named_scope('p14_wdone0'):
        w_arrived(0)
    with jax.named_scope('p15_x1'):
        for q in range(NX):
            for a in (0, 1):
                x_recv(a, 1, q)

    def part(lo, hi, h, first, n0=0, n1=NW):
        m = (hi - lo) * BLK

        def step(half, _):
            col = ((x + h) % 4) * 2048 + half * 1024
            xk = X[lo:hi, :, pl.ds(pl.multiple_of(col, 1024), 1024)].reshape(m, 1024)
            wkc = W[h, half, :, :, :, :, n0:n1].reshape(1024, n1 - n0)
            d = jnp.dot(xk, wkc, preferred_element_type=jnp.float32)
            if first:
                @pl.when(half == 0)
                def _():
                    acc[0:m, n0:n1] = d

                @pl.when(half > 0)
                def _():
                    acc[0:m, n0:n1] += d
            else:
                acc[0:m, n0:n1] += d
            return 0

        lax.fori_loop(0, 2, step, 0)

    def lines(e, us, first):
        h, sg = chunk_of(e), 1 - 2 * (e % 2)
        base = ((x + h) % 4) * 2048
        xs_, ws_ = [], []

        def cols(at, n):
            at = pl.multiple_of(at, n)
            xs_.append(X[0:3, :, pl.ds(at, n)].reshape(3 * BLK, n))

        for u in us:
            if e < 2:
                yy = (y + 4 + sg * u) % 4
                ws_.append(W[h, yy // 2, :, yy % 2].reshape(512, NW))
                for zz in range(4):
                    cols(base + (yy // 2) * 1024 + zz * 256 + (yy % 2) * 128, 128)
            else:
                zz = (z + 4 + sg * u) % 4
                ws_.append(W[h, :, zz].reshape(512, NW))
                for yy in range(2):
                    cols(base + yy * 1024 + zz * 256, 256)
        d = jnp.dot(
            jnp.concatenate(xs_, axis=1), jnp.concatenate(ws_, axis=0),
            preferred_element_type=jnp.float32,
        )
        if first:
            acc[...] = d
        else:
            acc[...] += d

    kv_cps = []

    def keep_kv(s, row):
        off = SLOT.index(s)
        i = (x + off) % 4
        ref = KV.at[2 * i + yh]
        ref[...] = acc[row : row + BLK, NQ:NW].astype(jnp.bfloat16)
        cp = pltpu.make_async_remote_copy(
            ref, ref, kvs.at[off], kvr.at[off], device_id=pair, device_id_type=MESH
        )
        cp.start()
        kv_cps.append(cp)

    def keep_q(s, row):
        i = (x + SLOT.index(s)) % 4
        Q[i] = acc[row : row + BLK, 0:NQ].astype(jnp.bfloat16)

    with jax.named_scope('p16_lines03'):
        for e in range(4):
            lines(e, (0, 3), e == 0)
            w_over([(u, 1, ()) for u in (0, 3, 1, 2)], e, e + 1)
    with jax.named_scope('p17_w6'):
        w_wave(6)
    with jax.named_scope('p17b_o1'):
        o_over([(3, 0, (0, 2, 3))])
    with jax.named_scope('p18_wdone1'):
        w_arrived(1)
    with jax.named_scope('p19_lines12'):
        for e in range(4):
            lines(e, (1, 2), False)
        for s in range(3):
            keep_kv(s, s * BLK)
            keep_q(s, s * BLK)
    with jax.named_scope('p21_proj1'):
        for q in range(NX):
            for a in (0, 1):
                x_recv(a, 2, q)
            h = (q - x + 4) % 4
            if q < NX - 1:
                part(3, 4, h, q == 0)
            else:
                part(3, 4, h, False, NQ, NW)
                keep_kv(3, 0)
                part(3, 4, h, False, 0, NQ)
                keep_q(3, 0)
    with jax.named_scope('p21b_o2'):
        o_over([(1, 0, (2, 3))])
    with jax.named_scope('p22_kv'):
        for off in range(4):
            i = (x + off) % 4
            ref = KV.at[2 * i + 1 - yh]
            pltpu.make_async_remote_copy(
                ref, ref, kvs.at[off], kvr.at[off], device_id=pair, device_id_type=MESH
            ).wait_recv()
    scale = HD ** (-0.5)

    def h_ref(j, a, u):
        sg = 1 - 2 * a
        return HG.at[j, (x + 4 + sg * u) % 4, 2 * a : 2 * a + 2]

    def h_send(j, a, u, k):
        sg = 1 - 2 * a
        r = 1 if k != 1 else -1
        ref = h_ref(j, a, u)
        pltpu.make_async_remote_copy(
            ref, ref, hs.at[k], hr.at[j, a, (u - r) % 4],
            device_id=at_x(r * sg), device_id_type=MESH,
        ).start()

    def h_recv(j, a, u):
        ref = h_ref(j, a, u)
        pltpu.make_async_remote_copy(
            ref, ref, hs.at[0], hr.at[j, a, u], device_id=sib, device_id_type=MESH
        ).wait_recv()

    def attend(j):
        rows = pl.ds(pl.multiple_of(j * 32, 32), 32)
        for i in range(4):
            nk = (2 * i + 2) * BLK
            q = jnp.concatenate(
                [Q[i, rows, h * HD : (h + 1) * HD] for h in range(8)], axis=0
            )
            kk = KV[0 : 2 * i + 2, :, 0:HD].reshape(nk, HD)
            vv = KV[0 : 2 * i + 2, :, HD:NKV].reshape(nk, HD)
            s = lax.dot_general(
                q, kk, (((1,), (1,)), ((), ())), preferred_element_type=jnp.float32
            ) * scale
            qpos = (2 * i + yh) * BLK + j * 32 + lax.broadcasted_iota(
                jnp.int32, (256, nk), 0
            ) % 32
            kpos = lax.broadcasted_iota(jnp.int32, (256, nk), 1)
            s = jnp.where(qpos >= kpos, s, jnp.float32(-1e30))
            e = jnp.exp(s - jnp.max(s, axis=-1, keepdims=True))
            pr = (e * (1.0 / jnp.sum(e, axis=-1, keepdims=True))).astype(jnp.bfloat16)
            o = jnp.dot(pr, vv, preferred_element_type=jnp.float32).astype(jnp.bfloat16)
            for h in range(8):
                HG[j, x, i, :, h * HD : (h + 1) * HD] = o[h * 32 : (h + 1) * 32]
            if i % 2:
                h_send(j, i // 2, 0, 0)
                h_send(j, i // 2, 0, 1)

    def h_forward(j):
        for a in (0, 1):
            h_recv(j, a, 3)
            h_send(j, a, 3, 2)

    with jax.named_scope('p24_attend'):
        attend(0)
        o_wave(2)
        attend(1)
        o_wave(3)
        attend(2)
        h_forward(0)
        attend(3)
        h_forward(1)
    with jax.named_scope('p25_o45'):
        o_wave(4)
        o_wave(5)
        o_wave(6)
    with jax.named_scope('p26_odone'):
        o_arrived(0)
        o_arrived(1)

    def out_ref(j, xx):
        return out.at[
            pl.ds(pl.multiple_of(j * 32, 32), 32), pl.ds(pl.multiple_of(xx * NO, NO), NO)
        ]

    def tile(j, n):
        t = jnp.zeros((BLK, 512), jnp.float32)
        for kc in range(8):
            wo = jnp.concatenate(
                [WO[8 * n + 2 * e + kc // 4, kc % 4] for e in range(4)], axis=1
            )
            lhs = HG[j, kc // 2, :, :, (kc % 2) * 512 : (kc % 2) * 512 + 512].reshape(BLK, 512)
            t += jnp.dot(lhs, wo, preferred_element_type=jnp.float32)
        OB[j, :, :, pl.ds(pl.multiple_of(n * 512, 512), 512)] = t.astype(
            jnp.bfloat16
        ).reshape(4, 32, 512)

    def mix(j, _):
        with jax.named_scope('m_wait'):
            for a in (0, 1):
                h_recv(j, a, 1)
                h_recv(j, a, 2)
        lax.fori_loop(0, 2, lambda n, _: (tile(j, n), 0)[1], 0)

        @pl.when(j < 2)
        def _():
            h_forward(j + 2)

        lax.fori_loop(2, 4, lambda n, _: (tile(j, n), 0)[1], 0)
        for r in (2, 1, 3):
            pltpu.make_async_remote_copy(
                OB.at[j, (x + r) % 4], out_ref(j, x), os_.at[r], or_.at[j, 4 - r],
                device_id=at_x(r), device_id_type=MESH,
            ).start()
        pltpu.make_async_copy(OB.at[j, x], out_ref(j, x), ol).start()
        return 0

    with jax.named_scope('p27_mix'):
        lax.fori_loop(0, 4, mix, 0)

    with jax.named_scope('p28_sent'):
        for cp in xsends + x_own + x_fwd + kv_cps:
            cp.wait_send()
    wo_swap.wait_send()
    w_sent()
    o_sent()
    for k in range(3):
        pltpu.make_async_remote_copy(
            HG.at[0], HG.at[0], hs.at[k], hs.at[k], device_id=sib, device_id_type=MESH
        ).wait_send()
    for r in (1, 2, 3):
        pltpu.make_async_remote_copy(
            OB.at[0], OB.at[0], os_.at[r], os_.at[r], device_id=sib, device_id_type=MESH
        ).wait_send()
    pltpu.make_async_copy(OB.at[0], OB.at[0], ol).wait()

    def finish(j, _):
        for r in (1, 2, 3):
            d = out_ref(j, (x + r) % 4)
            pltpu.make_async_remote_copy(
                d, d, os_.at[r], or_.at[j, r], device_id=sib, device_id_type=MESH
            ).wait_recv()
        return 0

    with jax.named_scope('p29_finish'):
        lax.fori_loop(0, 4, finish, 0)


def body(tokens, norm_gain, w_query, key_weight, value_weight, w_out):
    hbm = pl.BlockSpec(memory_space=pltpu.HBM)
    vmem = pl.BlockSpec(memory_space=pltpu.VMEM)
    bf = jnp.bfloat16
    dma = pltpu.SemaphoreType.DMA
    branch = pl.pallas_call(
        kernel,
        out_shape=jax.ShapeDtypeStruct((BLK, D), bf),
        in_specs=[hbm, vmem, hbm, hbm, hbm, hbm],
        out_specs=hbm,
        scratch_shapes=[
            pltpu.VMEM((4, 2, 4, 2, 2, 64, NW), bf),
            pltpu.VMEM((32, 4, 512, BLK), bf),
            pltpu.VMEM((4, BLK, D), bf),
            pltpu.VMEM((4, BLK, NQ), bf),
            pltpu.VMEM((8, BLK, NKV), bf),
            pltpu.VMEM((4, 4, 4, 32, NQ), bf),
            pltpu.VMEM((4, 4, 32, NO), bf),
            pltpu.VMEM((3 * BLK, NW), jnp.float32),
            pltpu.VMEM((2, 64, 2048), bf),
            dma((10,)), dma((4, 6)), dma((4, 6)), dma((2, 3, NX)), dma((2, 4, NX)),
            dma((5,)), dma((4, 4, 4)), dma((2,)),
            dma((5,)), dma((4, 4, 4)), dma((2,)),
            dma((4,)), dma((4,)), dma((3,)), dma((4, 2, 4)),
            dma((4,)), dma((4, 4)), dma(()),
        ],
        compiler_params=pltpu.CompilerParams(
            collective_id=0, has_side_effects=True, vmem_limit_bytes=67043328
        ),
        name="sublayer",
    )(tokens[0], norm_gain.reshape(1, D), w_query, key_weight, value_weight, w_out.T)
    return tokens.astype(jnp.float32) + branch[None].astype(jnp.float32)


def solution(mesh):
    placed = (
        P("fsdp", "seq", None),
        P(),
        P(("seq", "fsdp"), None),
        P(("seq", "fsdp"), None),
        P(("seq", "fsdp"), None),
        P(None, ("seq", "fsdp")),
    )
    return jax.shard_map(
        body, mesh=mesh, in_specs=placed, out_specs=P("fsdp", "seq", None), check_vma=False
    )
```

```python
import jax
import jax.numpy as jnp
from jax import lax
from jax.experimental import pallas as pl
from jax.experimental.pallas import tpu as pltpu
from jax.sharding import PartitionSpec as P

HD = 128
BLK = 128
D = 8192
NQ = 1024
NKV = 256
NW = NQ + NKV
NO = 2048
MESH = pl.DeviceIdType.MESH
SLOT = (0, 1, 3, 2)
NH = 640


def kernel(
    tok, gain, wq, wk, wv, wot, out,
    W, WO, XN, X, Q, KV, HG, OB, acc,
    T, PB, RB, loc, xs, xr, xss, xrs, pbs, rbr, wS, wR, wRD, oS, oR, oRD, kvs, kvr, hs, hr, os_, or_, ol,
):
    sx = lax.axis_index("seq")
    f = lax.axis_index("fsdp")
    x, yh = sx // 2, sx % 2
    z, yl, c = f // 4, (f // 2) % 2, f % 2
    y = 2 * yh + yl
    p = yh * 16 + f

    def dev(xx, yy, zz, cc):
        return (2 * xx + yy // 2, 4 * zz + 2 * (yy % 2) + cc)

    def at_x(r):
        return dev((x + r) % 4, y, z, c)

    sib = dev(x, y, z, 1 - c)
    pair = dev(x, (y + 2) % 4, z, c)

    barrier = pltpu.get_barrier_semaphore()
    peers = [at_x(1), at_x(2), at_x(3), sib, pair]
    peers += [dev(x, (y + 1) % 4, z, c), dev(x, (y + 3) % 4, z, c)]
    peers += [dev(x, y, (z + 1) % 4, c), dev(x, y, (z + 3) % 4, c)]
    for d in peers:
        pl.semaphore_signal(barrier, inc=1, device_id=d, device_id_type=MESH)

    def w_parts(t, h, make):
        def dst(g, s, lo, hi):
            return W.at[g, h, s, yh, z, yl, c, :, lo:hi]

        def wide(n, half):
            return wq.at[:, pl.ds(pl.multiple_of(n * NQ + half * 512, 512), 512)]

        def narrow(w, n):
            return w.at[:, pl.ds(pl.multiple_of(n * HD, HD), HD)]

        rem, own = [], []
        for m, d in ((0, 1), (1, 3)):
            n = (t + d) % 4
            rem.append((None, make(wide(n, t // 2), dst(0, m, 0, 512), 2 * m)))
            rem.append(
                (
                    t // 2,
                    make(narrow(wk, n), dst(0, m, 512, NH), 2 * m + 1),
                    make(narrow(wv, n), dst(0, m, 512, NH), 2 * m + 1),
                )
            )
        for s, w in ((0, wk), (1, wv)):
            own.append((None, make(wide(t, s), dst(1, s, 0, 512), 4 + 2 * s)))
            own.append((None, make(narrow(w, t), dst(1, s, 512, NH), 5 + 2 * s)))
        return rem, own

    def begin(part):
        if part[0] is None:
            part[1].start()
        else:
            for k in (0, 1):
                pl.when(part[0] == k)(part[1 + k].start)

    def local(s, d, k):
        return pltpu.make_async_copy(s, d, loc.at[4 + k])

    def remote(s, d, k):
        return pltpu.make_async_remote_copy(
            s, d, xs.at[k], xr.at[k], device_id=at_x(2), device_id_type=MESH
        )

    in_rem, in_own = w_parts(x, 0, local)
    for part in in_rem + in_own:
        begin(part)
    khalf = pl.ds(pl.multiple_of(c * 2048, 2048), 2048)
    other = pl.ds(pl.multiple_of((1 - c) * 2048, 2048), 2048)
    tok_in = pltpu.make_async_copy(tok, XN, loc.at[0])
    tok_in.start()
    wo_in = pltpu.make_async_copy(wot.at[:, khalf], T.at[c], loc.at[1])
    wo_in.start()

    with jax.named_scope('p01_barrier'):
        pl.semaphore_wait(barrier, len(peers))

    out_rem, out_own = w_parts((x + 2) % 4, 1, remote)
    for part in out_rem + out_own:
        begin(part)
    wo_swap = pltpu.make_async_remote_copy(
        wot.at[:, other], T.at[c], loc.at[2], loc.at[3], device_id=sib, device_id_type=MESH
    )
    wo_swap.start()

    got_rem, got_own = w_parts(x, 1, remote)

    def gather(S, R, RD, piece, many):
        def coords(h, a1, a2):
            g, sg = h // 2, 1 - 2 * (h % 2)
            yy = (y + 4 + sg * (a1 * g + a2 * (1 - g))) % 4
            zz = (z + 4 + sg * (a1 * (1 - g) + a2 * g)) % 4
            return yy, zz

        def ref(h, u1, u2):
            yy, zz = coords(h, u1, u2)
            return piece(h, yy, zz)

        def send(h, u1, u2, k):
            a1, a2 = ((1, 0), (-1, 0), (0, 1), (0, -1))[k]
            yy, zz = coords(h, a1, a2)
            r = ref(h, u1, u2)
            pltpu.make_async_remote_copy(
                r, r, S.at[k], R.at[h, (u1 - a1) % 4, (u2 - a2) % 4],
                device_id=dev(x, yy, zz, c), device_id_type=MESH,
            ).start()

        def across(h, u1, u2):
            r = ref(h, u1, u2)
            pltpu.make_async_remote_copy(
                r, r, S.at[4], RD.at[int(u2 == 2)], device_id=sib, device_id_type=MESH
            ).start()

        def recv(h, u1, u2):
            r = ref(h, u1, u2)
            pltpu.make_async_remote_copy(
                r, r, S.at[4], R.at[h, u1, u2], device_id=sib, device_id_type=MESH
            ).wait_recv()

        def over_pieces(steps, first=0, last=4, again=False):
            def one(h, _):
                for u1, u2, ks in steps:
                    if not again and (u1, u2) != (0, 0):
                        recv(h, u1, u2)
                    for k in ks:
                        send(h, u1, u2, k)
                    if not again:
                        across(h, u1, u2)
                return 0

            lax.fori_loop(first, last, one, 0)

        def whole(sem, n):
            return pltpu.make_async_remote_copy(
                many(n), many(n), sem, sem, device_id=sib, device_id_type=MESH
            )

        def wave(n):
            if n == 1:
                over_pieces([(3, 0, (0,))])
                over_pieces([(3, 0, (2, 3))], again=True)
                over_pieces([(1, 0, (2, 3))])
            elif n == 2:
                over_pieces([(2, 0, (2, 3)), (0, 3, (2,))])
            elif n == 3:
                over_pieces([(3, 3, (2,)), (1, 3, (2,))])
            elif n == 4:
                over_pieces([(2, 3, (2,))])
            elif n == 5:
                over_pieces([(u, 1, ()) for u in (0, 3, 1, 2)])
            elif n == 6:
                over_pieces([(u, 2, ()) for u in (0, 3, 1, 2)])

        def arrived(k):
            whole(RD.at[k], (48, 16)[k]).wait_recv()

        def sent():
            for k, n in enumerate((8, 4, 32, 16, 64)):
                whole(S.at[k], n).wait_send()

        return over_pieces, wave, arrived, sent

    def w_many(n):
        if n == 64:
            return W.at[0, 0]
        if n == 48:
            return W.at[0, 0, :, :, 0:3]
        if n == 32:
            return W.at[0, 0, 0]
        if n == 16:
            return W.at[0, 0, 0, 0]
        return W.at[0, 0, 0, 0, 0 : n // 4]

    def w_gather(g):
        return gather(
            wS.at[g], wR.at[g], wRD.at[g],
            lambda e, yy, zz: W.at[g, e % 2, e // 2, yy // 2, zz, yy % 2, c],
            w_many,
        )

    r_over, r_wave, r_arrived, r_sent = w_gather(0)
    w_over, w_wave, w_arrived, w_sent = w_gather(1)
    o_over, o_wave, o_arrived, o_sent = gather(
        oS, oR, oRD,
        lambda e, yy, zz: WO.at[(yy // 2) * 16 + 4 * zz + 2 * (yy % 2) + c, e],
        lambda n: WO.at[0 : n // 4],
    )

    own = [(0, 0, (0, 1, 2, 3))]

    def each(over, steps, pieces):
        for e in pieces:
            over(steps, e, e + 1)

    with jax.named_scope('p02_r0a'):
        for part in in_rem:
            part[1].wait()
        each(r_over, own, (0, 2))

    with jax.named_scope('p02_tok'):
        tok_in.wait()

    def norm(r, _):
        rows = pl.ds(pl.multiple_of(r * 16, 16), 16)
        v = XN[rows, :].astype(jnp.float32)
        ms = jnp.mean(v * v, axis=-1, keepdims=True)
        XN[rows, :] = (v * lax.rsqrt(ms + 1e-05) * gain[...]).astype(jnp.bfloat16)
        return 0

    with jax.named_scope('p03_norm'):
        lax.fori_loop(0, BLK // 16, norm, 0)

    def x_cols(ch):
        return pl.ds(pl.multiple_of((ch % 4) * 2048, 2048), 2048)

    def x_copy(r, h):
        o = (4 - r) % 4
        return pltpu.make_async_remote_copy(
            XN.at[:, x_cols(x + r + 2 * h)], X.at[h, SLOT[o]], xss.at[r, h], xrs.at[o, h],
            device_id=at_x(r), device_id_type=MESH,
        )

    def x_recv(o, h):
        d = X.at[h, SLOT[o]]
        pltpu.make_async_remote_copy(
            d, d, xss.at[0, 0], xrs.at[o, h], device_id=sib, device_id_type=MESH
        ).wait_recv()

    x_sends = [x_copy(r, h) for rs in ((1, 3), (2,)) for h in (0, 1) for r in rs]
    for cp in x_sends:
        cp.start()
    for h in (0, 1):
        X[h, 0] = XN[:, x_cols(x + 2 * h)]

    with jax.named_scope('p04_swap'):
        wo_in.wait()
        wo_swap.wait_recv()
        t = T[...].reshape(BLK, 2048)
        for h in range(4):
            WO[p, h] = t[:, 512 * h : 512 * (h + 1)].T

    with jax.named_scope('p05_w0a'):
        for part in in_own:
            part[1].wait()
        each(w_over, own, (0, 2))
    with jax.named_scope('p06_r0b'):
        for part in got_rem:
            part[1].wait_recv()
        each(r_over, own, (1, 3))
    with jax.named_scope('p07_r1'):
        r_wave(1)
    with jax.named_scope('p08_w0b'):
        for part in got_own:
            part[1].wait_recv()
        each(w_over, own, (1, 3))
    with jax.named_scope('p09_r2'):
        r_wave(2)
    with jax.named_scope('p10_r3'):
        r_wave(3)
    with jax.named_scope('p11_r4'):
        r_wave(4)
    with jax.named_scope('p12_w1'):
        w_wave(1)
    with jax.named_scope('p13_r56'):
        r_wave(5)
        r_wave(6)
    with jax.named_scope('p14_w2'):
        w_wave(2)
    with jax.named_scope('p14_w3'):
        w_wave(3)
    with jax.named_scope('p15_rdone'):
        r_arrived(0)
        r_arrived(1)
    with jax.named_scope('p15_x1'):
        for o in (1, 3):
            for h in (0, 1):
                x_recv(o, h)

    def product(g, lo, hi, n0, n1, step):
        h, k = step // 2, step % 2
        wkc = jnp.concatenate(
            [W[g, h, t, k, :, :, :, :, n0:n1].reshape(1024, n1 - n0) for t in (0, 1)], axis=1
        )
        return jnp.dot(
            X[h, lo:hi, :, k * 1024 : (k + 1) * 1024].reshape((hi - lo) * BLK, 1024), wkc,
            preferred_element_type=jnp.float32,
        )

    def add_up(g, lo, hi, n0, n1, steps=(0, 1, 2, 3)):
        rows = slice(lo * BLK, hi * BLK)
        for step in steps:
            d = product(g, lo, hi, n0, n1, step)
            for t in (0, 1):
                cols = slice(t * NH + n0, t * NH + n1)
                part = d[:, t * (n1 - n0) : (t + 1) * (n1 - n0)]
                if step == 0:
                    acc[rows, cols] = part
                else:
                    acc[rows, cols] += part

    pb_cps = []

    def pb_send(s, n0, n1):
        i = (x + SLOT.index(s)) % 4
        for m, r in ((0, 1), (1, 3)):
            PB[s, m, :, n0:n1] = acc[
                s * BLK : (s + 1) * BLK, m * NH + n0 : m * NH + n1
            ].astype(jnp.bfloat16)
            cp = pltpu.make_async_remote_copy(
                PB.at[s, m, :, n0:n1], RB.at[x // 2, i, :, n0:n1],
                pbs.at[s, m, n0 // 512], rbr.at[x // 2, i, n0 // 512],
                device_id=at_x(r), device_id_type=MESH,
            )
            cp.start()
            pb_cps.append(cp)

    def rb_recv(n0, n1):
        for b in (0, 1):
            for i in range(4):
                ref = RB.at[b, i, :, n0:n1]
                pltpu.make_async_remote_copy(
                    ref, ref, pbs.at[0, 0, 0], rbr.at[b, i, n0 // 512],
                    device_id=sib, device_id_type=MESH,
                ).wait_recv()

    with jax.named_scope('p16_rem3a'):
        add_up(0, 0, 3, 0, NH, (0, 1))
    with jax.named_scope('p16_w4'):
        w_wave(4)
    with jax.named_scope('p16_rem3b'):
        add_up(0, 0, 3, 0, NH, (2, 3))
        for s in range(3):
            pb_send(s, 512, NH)
        for s in range(2):
            pb_send(s, 0, 512)
    with jax.named_scope('p16_o0'):
        o_over([(0, 0, (0, 1))], 0, 2)
        o_over(own, 2, 4)
        o_over([(0, 0, (2, 3))], 0, 1, True)
    with jax.named_scope('p16_w5'):
        w_wave(5)
    with jax.named_scope('p17_x2'):
        for h in (0, 1):
            x_recv(2, h)
    with jax.named_scope('p17_rem1'):
        add_up(0, 3, 4, 512, NH)
        pb_send(3, 512, NH)
        pb_send(2, 0, 512)
        add_up(0, 3, 4, 0, 512)
        pb_send(3, 0, 512)
    with jax.named_scope('p18_w6'):
        w_wave(6)
    with jax.named_scope('p18_wdone'):
        w_arrived(0)
        w_arrived(1)
    with jax.named_scope('p19_kv'):
        add_up(1, 0, 4, 512, NH)
    with jax.named_scope('p20_rbkv'):
        rb_recv(512, NH)

    kv_cps = []

    def total(s, b, lo, hi):
        i = (x + SLOT.index(s)) % 4
        t = acc[s * BLK : (s + 1) * BLK, b * NH + lo : b * NH + hi]
        return (t + RB[b, i, :, lo:hi].astype(jnp.float32)).astype(jnp.bfloat16)

    with jax.named_scope('p20_keepkv'):
        for s in range(4):
            off = SLOT.index(s)
            ref = KV.at[2 * ((x + off) % 4) + yh]
            ref[:, 0:HD] = total(s, 0, 512, NH)
            ref[:, HD:NKV] = total(s, 1, 512, NH)
            cp = pltpu.make_async_remote_copy(
                ref, ref, kvs.at[off], kvr.at[off], device_id=pair, device_id_type=MESH
            )
            cp.start()
            kv_cps.append(cp)
    with jax.named_scope('p20_o'):
        o_over([(3, 0, (0,))], 0, 2)
        o_over([(3, 0, (0, 2, 3)), (1, 0, (2, 3))], 2, 4)
        o_over([(0, 0, (2, 3))], 1, 2, True)
        o_over([(3, 0, (2, 3))], 0, 2, True)
        o_over([(1, 0, (2, 3))], 0, 2)
    with jax.named_scope('p21_q'):
        add_up(1, 0, 4, 0, 512)
    with jax.named_scope('p21_rbq'):
        rb_recv(0, 512)
    with jax.named_scope('p21_keepq'):
        for s in range(4):
            i = (x + SLOT.index(s)) % 4
            Q[i, :, 0:512] = total(s, 0, 0, 512)
            Q[i, :, 512:NQ] = total(s, 1, 0, 512)
    with jax.named_scope('p22_kv'):
        for off in range(4):
            i = (x + off) % 4
            ref = KV.at[2 * i + 1 - yh]
            pltpu.make_async_remote_copy(
                ref, ref, kvs.at[off], kvr.at[off], device_id=pair, device_id_type=MESH
            ).wait_recv()
    scale = HD ** (-0.5)

    def h_ref(j, a, u):
        sg = 1 - 2 * a
        return HG.at[j, (x + 4 + sg * u) % 4, 2 * a : 2 * a + 2]

    def h_send(j, a, u, k):
        sg = 1 - 2 * a
        r = 1 if k != 1 else -1
        ref = h_ref(j, a, u)
        pltpu.make_async_remote_copy(
            ref, ref, hs.at[k], hr.at[j, a, (u - r) % 4],
            device_id=at_x(r * sg), device_id_type=MESH,
        ).start()

    def h_recv(j, a, u):
        ref = h_ref(j, a, u)
        pltpu.make_async_remote_copy(
            ref, ref, hs.at[0], hr.at[j, a, u], device_id=sib, device_id_type=MESH
        ).wait_recv()

    def attend(j):
        rows = pl.ds(pl.multiple_of(j * 32, 32), 32)
        for i in range(4):
            nk = (2 * i + 2) * BLK
            q = jnp.concatenate(
                [Q[i, rows, h * HD : (h + 1) * HD] for h in range(8)], axis=0
            )
            kk = KV[0 : 2 * i + 2, :, 0:HD].reshape(nk, HD)
            vv = KV[0 : 2 * i + 2, :, HD:NKV].reshape(nk, HD)
            s = lax.dot_general(
                q, kk, (((1,), (1,)), ((), ())), preferred_element_type=jnp.float32
            ) * scale
            qpos = (2 * i + yh) * BLK + j * 32 + lax.broadcasted_iota(
                jnp.int32, (256, nk), 0
            ) % 32
            kpos = lax.broadcasted_iota(jnp.int32, (256, nk), 1)
            s = jnp.where(qpos >= kpos, s, jnp.float32(-1e30))
            e = jnp.exp(s - jnp.max(s, axis=-1, keepdims=True))
            pr = (e * (1.0 / jnp.sum(e, axis=-1, keepdims=True))).astype(jnp.bfloat16)
            o = jnp.dot(pr, vv, preferred_element_type=jnp.float32).astype(jnp.bfloat16)
            for h in range(8):
                HG[j, x, i, :, h * HD : (h + 1) * HD] = o[h * 32 : (h + 1) * 32]
            if i % 2:
                h_send(j, i // 2, 0, 0)
                h_send(j, i // 2, 0, 1)

    def h_forward(j):
        for a in (0, 1):
            h_recv(j, a, 3)
            h_send(j, a, 3, 2)

    with jax.named_scope('p24_attend0'):
        attend(0)
    with jax.named_scope('p24_o3'):
        o_over([(0, 3, (2,)), (2, 0, (2, 3)), (3, 3, (2,))], 2, 4)
    with jax.named_scope('p24_p_attend1'):
        attend(1)
    with jax.named_scope('p24b_o4'):
        o_over([(2, 0, (2, 3)), (0, 3, (2,))], 0, 2)
        o_over([(1, 3, (2,))], 2, 4)
    with jax.named_scope('p24c_attend2'):
        attend(2)
    with jax.named_scope('p24d_hf0'):
        h_forward(0)
    with jax.named_scope('p24e_attend3'):
        attend(3)
    with jax.named_scope('p24e_o5'):
        o_over([(2, 3, (2,))], 2, 4)
    with jax.named_scope('p24f_hf1'):
        h_forward(1)
    with jax.named_scope('p24g_o6'):
        o_over([(3, 3, (2,)), (1, 3, (2,))], 0, 2)
    with jax.named_scope('p24g_hf2'):
        h_forward(2)
    with jax.named_scope('p24h_o7'):
        o_over([(2, 3, (2,))], 0, 2)
    with jax.named_scope('p25_o5'):
        o_wave(5)
    with jax.named_scope('p26_odone0'):
        o_arrived(0)

    def out_ref(j, xx):
        return out.at[
            pl.ds(pl.multiple_of(j * 32, 32), 32), pl.ds(pl.multiple_of(xx * NO, NO), NO)
        ]

    order = [(0, 0), (0, 1), (0, 3), (1, 0), (1, 1), (1, 3), (3, 0), (3, 1)]
    order += [(3, 3), (0, 2), (1, 2), (3, 2), (2, 0), (2, 1), (2, 2), (2, 3)]

    def chip_at(q):
        yy, zz = (y + order[q][0]) % 4, (z + order[q][1]) % 4
        return (yy // 2) * 8 + 2 * zz + yy % 2

    def tile(j, n):
        t = jnp.zeros((BLK, 512), jnp.float32)
        for kc in range(8):
            wo = jnp.concatenate(
                [WO[2 * chip_at(4 * n + e) + kc // 4, kc % 4] for e in range(4)], axis=1
            )
            lhs = HG[j, kc // 2, :, :, (kc % 2) * 512 : (kc % 2) * 512 + 512].reshape(BLK, 512)
            t += jnp.dot(lhs, wo, preferred_element_type=jnp.float32)
        OB[j, :, :, n * 512 : (n + 1) * 512] = t.astype(jnp.bfloat16).reshape(4, 32, 512)
        for q in range(4 * n, 4 * n + 4):
            col = pl.multiple_of(x * NO + chip_at(q) * BLK, BLK)
            dst = out.at[pl.ds(pl.multiple_of(j * 32, 32), 32), pl.ds(col, BLK)]
            cols = slice(q * BLK, (q + 1) * BLK)
            for r in (2, 1, 3):
                pltpu.make_async_remote_copy(
                    OB.at[j, (x + r) % 4, :, cols], dst, os_.at[r], or_.at[j, 4 - r],
                    device_id=at_x(r), device_id_type=MESH,
                ).start()
            pltpu.make_async_copy(OB.at[j, x, :, cols], dst, ol).start()

    def early(j, _):
        with jax.named_scope('m_wait'):
            for a in (0, 1):
                h_recv(j, a, 1)
                h_recv(j, a, 2)
        tile(j, 0)
        tile(j, 1)
        return 0

    def late(j, _):
        tile(j, 2)
        tile(j, 3)
        return 0

    with jax.named_scope('p27_mix0'):
        lax.fori_loop(0, 1, early, 0)
    with jax.named_scope('p27_mix0_hf3'):
        h_forward(3)
    with jax.named_scope('p27_mix12'):
        lax.fori_loop(1, 3, early, 0)
    with jax.named_scope('p27_o6'):
        o_wave(6)
    with jax.named_scope('p27_p_mix3'):
        lax.fori_loop(3, 4, early, 0)
    with jax.named_scope('p27_q_odone1'):
        o_arrived(1)
    with jax.named_scope('p27_r_late'):
        lax.fori_loop(0, 4, late, 0)

    with jax.named_scope('p28_sent'):
        for cp in x_sends + pb_cps + kv_cps:
            cp.wait_send()
        for part in out_rem + out_own:
            part[1].wait_send()
    wo_swap.wait_send()
    r_sent()
    w_sent()
    o_sent()
    for k in range(3):
        pltpu.make_async_remote_copy(
            HG.at[0], HG.at[0], hs.at[k], hs.at[k], device_id=sib, device_id_type=MESH
        ).wait_send()
    for r in (1, 2, 3):
        pltpu.make_async_remote_copy(
            OB.at[0], OB.at[0], os_.at[r], os_.at[r], device_id=sib, device_id_type=MESH
        ).wait_send()
    pltpu.make_async_copy(OB.at[0], OB.at[0], ol).wait()

    def finish(j, _):
        for r in (1, 2, 3):
            d = out_ref(j, (x + r) % 4)
            pltpu.make_async_remote_copy(
                d, d, os_.at[r], or_.at[j, r], device_id=sib, device_id_type=MESH
            ).wait_recv()
        return 0

    with jax.named_scope('p29_finish'):
        lax.fori_loop(0, 4, finish, 0)


def body(tokens, norm_gain, w_query, key_weight, value_weight, w_out):
    hbm = pl.BlockSpec(memory_space=pltpu.HBM)
    vmem = pl.BlockSpec(memory_space=pltpu.VMEM)
    bf = jnp.bfloat16
    dma = pltpu.SemaphoreType.DMA
    branch = pl.pallas_call(
        kernel,
        out_shape=jax.ShapeDtypeStruct((BLK, D), bf),
        in_specs=[hbm, vmem, hbm, hbm, hbm, hbm],
        out_specs=hbm,
        scratch_shapes=[
            pltpu.VMEM((2, 2, 2, 2, 4, 2, 2, 64, NH), bf),
            pltpu.VMEM((32, 4, 512, BLK), bf),
            pltpu.VMEM((BLK, D), bf),
            pltpu.VMEM((2, 4, BLK, 2048), bf),
            pltpu.VMEM((4, BLK, NQ), bf),
            pltpu.VMEM((8, BLK, NKV), bf),
            pltpu.VMEM((4, 4, 4, 32, NQ), bf),
            pltpu.VMEM((4, 4, 32, NO), bf),
            pltpu.VMEM((4 * BLK, NW), jnp.float32),
            pltpu.VMEM((2, 64, 2048), bf),
            pltpu.VMEM((4, 2, BLK, NH), bf),
            pltpu.VMEM((2, 4, BLK, NH), bf),
            dma((12,)), dma((8,)), dma((8,)), dma((4, 2)), dma((4, 2)), dma((4, 2, 2)), dma((2, 4, 2)),
            dma((2, 5)), dma((2, 4, 4, 4)), dma((2, 2)),
            dma((5,)), dma((4, 4, 4)), dma((2,)),
            dma((4,)), dma((4,)), dma((3,)), dma((4, 2, 4)),
            dma((4,)), dma((4, 4)), dma(()),
        ],
        compiler_params=pltpu.CompilerParams(
            collective_id=0, has_side_effects=True, vmem_limit_bytes=60600000
        ),
        name="sublayer",
    )(tokens[0], norm_gain.reshape(1, D), w_query, key_weight, value_weight, w_out.T)
    return tokens.astype(jnp.float32) + branch[None].astype(jnp.float32)


def solution(mesh):
    placed = (
        P("fsdp", "seq", None),
        P(),
        P(("seq", "fsdp"), None),
        P(("seq", "fsdp"), None),
        P(("seq", "fsdp"), None),
        P(None, ("seq", "fsdp")),
    )
    return jax.shard_map(
        body, mesh=mesh, in_specs=placed, out_specs=P("fsdp", "seq", None), check_vma=False
    )
```

```python
import jax
import jax.numpy as jnp
from jax import lax
from jax.experimental import pallas as pl
from jax.experimental.pallas import tpu as pltpu
from jax.sharding import PartitionSpec as P

HD = 128
BLK = 128
D = 8192
NQ = 1024
NKV = 256
NW = NQ + NKV
NO = 2048
MESH = pl.DeviceIdType.MESH
SLOT = (0, 1, 3, 2)
NH = 640


def kernel(
    tok, gain, wq, wk, wv, wot, out,
    W, WO, XN, X, Q, KV, HG, OB, acc,
    T, PB, RB, loc, xs, xr, xss, xrs, pbs, rbr, wS, wR, wRD, oS, oR, oRD, kvs, kvr, hs, hr, os_, or_, ol,
):
    sx = lax.axis_index("seq")
    f = lax.axis_index("fsdp")
    x, yh = sx // 2, sx % 2
    z, yl, c = f // 4, (f // 2) % 2, f % 2
    y = 2 * yh + yl
    p = yh * 16 + f

    def dev(xx, yy, zz, cc):
        return (2 * xx + yy // 2, 4 * zz + 2 * (yy % 2) + cc)

    def at_x(r):
        return dev((x + r) % 4, y, z, c)

    sib = dev(x, y, z, 1 - c)
    pair = dev(x, (y + 2) % 4, z, c)

    barrier = pltpu.get_barrier_semaphore()
    peers = [at_x(1), at_x(2), at_x(3), sib, pair]
    peers += [dev(x, (y + 1) % 4, z, c), dev(x, (y + 3) % 4, z, c)]
    peers += [dev(x, y, (z + 1) % 4, c), dev(x, y, (z + 3) % 4, c)]
    for d in peers:
        pl.semaphore_signal(barrier, inc=1, device_id=d, device_id_type=MESH)

    def w_parts(t, h, make):
        def dst(g, s, lo, hi):
            return W.at[g, h, s, yh, z, yl, c, :, lo:hi]

        def wide(n, half):
            return wq.at[:, pl.ds(pl.multiple_of(n * NQ + half * 512, 512), 512)]

        def narrow(w, n):
            return w.at[:, pl.ds(pl.multiple_of(n * HD, HD), HD)]

        rem, own = [], []
        for m, d in ((0, 1), (1, 3)):
            n = (t + d) % 4
            rem.append((None, make(wide(n, t // 2), dst(0, m, 0, 512), 2 * m)))
            rem.append(
                (
                    t // 2,
                    make(narrow(wk, n), dst(0, m, 512, NH), 2 * m + 1),
                    make(narrow(wv, n), dst(0, m, 512, NH), 2 * m + 1),
                )
            )
        for s, w in ((0, wk), (1, wv)):
            own.append((None, make(wide(t, s), dst(1, s, 0, 512), 4 + 2 * s)))
            own.append((None, make(narrow(w, t), dst(1, s, 512, NH), 5 + 2 * s)))
        return rem, own

    def begin(part):
        if part[0] is None:
            part[1].start()
        else:
            for k in (0, 1):
                pl.when(part[0] == k)(part[1 + k].start)

    def local(s, d, k):
        return pltpu.make_async_copy(s, d, loc.at[4 + k])

    def remote(s, d, k):
        return pltpu.make_async_remote_copy(
            s, d, xs.at[k], xr.at[k], device_id=at_x(2), device_id_type=MESH
        )

    in_rem, in_own = w_parts(x, 0, local)
    for part in in_rem + in_own:
        begin(part)
    khalf = pl.ds(pl.multiple_of(c * 2048, 2048), 2048)
    other = pl.ds(pl.multiple_of((1 - c) * 2048, 2048), 2048)
    tok_in = pltpu.make_async_copy(tok, XN, loc.at[0])
    tok_in.start()
    wo_in = pltpu.make_async_copy(wot.at[:, khalf], T.at[c], loc.at[1])
    wo_in.start()

    with jax.named_scope('p01_barrier'):
        pl.semaphore_wait(barrier, len(peers))

    out_rem, out_own = w_parts((x + 2) % 4, 1, remote)
    for part in out_rem + out_own:
        begin(part)
    wo_swap = pltpu.make_async_remote_copy(
        wot.at[:, other], T.at[c], loc.at[2], loc.at[3], device_id=sib, device_id_type=MESH
    )
    wo_swap.start()

    got_rem, got_own = w_parts(x, 1, remote)

    def gather(S, R, RD, piece, many):
        def coords(h, a1, a2):
            g, sg = h // 2, 1 - 2 * (h % 2)
            yy = (y + 4 + sg * (a1 * g + a2 * (1 - g))) % 4
            zz = (z + 4 + sg * (a1 * (1 - g) + a2 * g)) % 4
            return yy, zz

        def ref(h, u1, u2):
            yy, zz = coords(h, u1, u2)
            return piece(h, yy, zz)

        def send(h, u1, u2, k):
            a1, a2 = ((1, 0), (-1, 0), (0, 1), (0, -1))[k]
            yy, zz = coords(h, a1, a2)
            r = ref(h, u1, u2)
            pltpu.make_async_remote_copy(
                r, r, S.at[k], R.at[h, (u1 - a1) % 4, (u2 - a2) % 4],
                device_id=dev(x, yy, zz, c), device_id_type=MESH,
            ).start()

        def across(h, u1, u2):
            r = ref(h, u1, u2)
            pltpu.make_async_remote_copy(
                r, r, S.at[4], RD.at[int(u2 == 2)], device_id=sib, device_id_type=MESH
            ).start()

        def recv(h, u1, u2):
            r = ref(h, u1, u2)
            pltpu.make_async_remote_copy(
                r, r, S.at[4], R.at[h, u1, u2], device_id=sib, device_id_type=MESH
            ).wait_recv()

        def over_pieces(steps, first=0, last=4, again=False):
            def one(h, _):
                for u1, u2, ks in steps:
                    if not again and (u1, u2) != (0, 0):
                        recv(h, u1, u2)
                    for k in ks:
                        send(h, u1, u2, k)
                    if not again:
                        across(h, u1, u2)
                return 0

            lax.fori_loop(first, last, one, 0)

        def whole(sem, n):
            return pltpu.make_async_remote_copy(
                many(n), many(n), sem, sem, device_id=sib, device_id_type=MESH
            )

        def wave(n):
            if n == 1:
                over_pieces([(3, 0, (0,))])
                over_pieces([(3, 0, (2, 3))], again=True)
                over_pieces([(1, 0, (2, 3))])
            elif n == 2:
                over_pieces([(2, 0, (2, 3)), (0, 3, (2,))])
            elif n == 3:
                over_pieces([(3, 3, (2,)), (1, 3, (2,))])
            elif n == 4:
                over_pieces([(2, 3, (2,))])
            elif n == 5:
                over_pieces([(u, 1, ()) for u in (0, 3, 1, 2)])
            elif n == 6:
                over_pieces([(u, 2, ()) for u in (0, 3, 1, 2)])

        def arrived(k):
            whole(RD.at[k], (48, 16)[k]).wait_recv()

        def sent():
            for k, n in enumerate((8, 4, 32, 16, 64)):
                whole(S.at[k], n).wait_send()

        return over_pieces, wave, arrived, sent

    def w_many(n):
        if n == 64:
            return W.at[0, 0]
        if n == 48:
            return W.at[0, 0, :, :, 0:3]
        if n == 32:
            return W.at[0, 0, 0]
        if n == 16:
            return W.at[0, 0, 0, 0]
        return W.at[0, 0, 0, 0, 0 : n // 4]

    def w_gather(g):
        return gather(
            wS.at[g], wR.at[g], wRD.at[g],
            lambda e, yy, zz: W.at[g, e % 2, e // 2, yy // 2, zz, yy % 2, c],
            w_many,
        )

    r_over, r_wave, r_arrived, r_sent = w_gather(0)
    w_over, w_wave, w_arrived, w_sent = w_gather(1)
    o_over, o_wave, o_arrived, o_sent = gather(
        oS, oR, oRD,
        lambda e, yy, zz: WO.at[(yy // 2) * 16 + 4 * zz + 2 * (yy % 2) + c, e],
        lambda n: WO.at[0 : n // 4],
    )

    own = [(0, 0, (0, 1, 2, 3))]

    def each(over, steps, pieces):
        for e in pieces:
            over(steps, e, e + 1)

    with jax.named_scope('p02_r0a'):
        for part in in_rem:
            part[1].wait()
        each(r_over, own, (0, 2))

    with jax.named_scope('p02_tok'):
        tok_in.wait()

    def norm(r, _):
        rows = pl.ds(pl.multiple_of(r * 16, 16), 16)
        v = XN[rows, :].astype(jnp.float32)
        ms = jnp.mean(v * v, axis=-1, keepdims=True)
        XN[rows, :] = (v * lax.rsqrt(ms + 1e-05) * gain[...]).astype(jnp.bfloat16)
        return 0

    with jax.named_scope('p03_norm'):
        lax.fori_loop(0, BLK // 16, norm, 0)

    def x_cols(ch):
        return pl.ds(pl.multiple_of((ch % 4) * 2048, 2048), 2048)

    def x_copy(r, h):
        o = (4 - r) % 4
        return pltpu.make_async_remote_copy(
            XN.at[:, x_cols(x + r + 2 * h)], X.at[h, SLOT[o]], xss.at[r, h], xrs.at[o, h],
            device_id=at_x(r), device_id_type=MESH,
        )

    def x_recv(o, h):
        d = X.at[h, SLOT[o]]
        pltpu.make_async_remote_copy(
            d, d, xss.at[0, 0], xrs.at[o, h], device_id=sib, device_id_type=MESH
        ).wait_recv()

    x_sends = [x_copy(r, h) for rs in ((1, 3), (2,)) for h in (0, 1) for r in rs]
    for cp in x_sends:
        cp.start()
    for h in (0, 1):
        X[h, 0] = XN[:, x_cols(x + 2 * h)]

    with jax.named_scope('p04_swap'):
        wo_in.wait()
        wo_swap.wait_recv()
        t = T[...].reshape(BLK, 2048)
        for h in range(4):
            WO[p, h] = t[:, 512 * h : 512 * (h + 1)].T

    with jax.named_scope('p05_w0a'):
        for part in in_own:
            part[1].wait()
        each(w_over, own, (0, 2))
    with jax.named_scope('p06_r0b'):
        for part in got_rem:
            part[1].wait_recv()
        each(r_over, own, (1, 3))
    with jax.named_scope('p07_r1'):
        r_wave(1)
    with jax.named_scope('p08_w0b'):
        for part in got_own:
            part[1].wait_recv()
        each(w_over, own, (1, 3))
    with jax.named_scope('p09_r2'):
        r_wave(2)
    with jax.named_scope('p10_r3'):
        r_wave(3)
    with jax.named_scope('p11_r4'):
        r_wave(4)
    with jax.named_scope('p12_w1'):
        w_wave(1)
    with jax.named_scope('p13_r56'):
        r_wave(5)
        r_wave(6)
    with jax.named_scope('p14_w2'):
        w_wave(2)
    with jax.named_scope('p14_w3'):
        w_wave(3)
    with jax.named_scope('p15_rdone'):
        r_arrived(0)
        r_arrived(1)
    with jax.named_scope('p15_x1'):
        for o in (1, 3):
            for h in (0, 1):
                x_recv(o, h)

    def add_up(g, lo, hi, n0, n1, chunks=(0, 1)):
        rows = slice(lo * BLK, hi * BLK)
        n = n1 - n0
        for h in chunks:
            wkc = jnp.concatenate(
                [W[g, h, t, :, :, :, :, :, n0:n1].reshape(2048, n) for t in (0, 1)], axis=1
            )
            d = jnp.dot(
                X[h, lo:hi].reshape((hi - lo) * BLK, 2048), wkc,
                preferred_element_type=jnp.float32,
            )
            for t in (0, 1):
                cols = slice(t * NH + n0, t * NH + n1)
                part = d[:, t * n : (t + 1) * n]
                if h == 0:
                    acc[rows, cols] = part
                else:
                    acc[rows, cols] += part

    pb_cps = []

    def pb_send(s, n0, n1):
        i = (x + SLOT.index(s)) % 4
        for m, r in ((0, 1), (1, 3)):
            PB[s, m, :, n0:n1] = acc[
                s * BLK : (s + 1) * BLK, m * NH + n0 : m * NH + n1
            ].astype(jnp.bfloat16)
            cp = pltpu.make_async_remote_copy(
                PB.at[s, m, :, n0:n1], RB.at[x // 2, i, :, n0:n1],
                pbs.at[s, m, n0 // 512], rbr.at[x // 2, i, n0 // 512],
                device_id=at_x(r), device_id_type=MESH,
            )
            cp.start()
            pb_cps.append(cp)

    def rb_recv(n0, n1):
        for b in (0, 1):
            for i in range(4):
                ref = RB.at[b, i, :, n0:n1]
                pltpu.make_async_remote_copy(
                    ref, ref, pbs.at[0, 0, 0], rbr.at[b, i, n0 // 512],
                    device_id=sib, device_id_type=MESH,
                ).wait_recv()

    with jax.named_scope('p16_rem3a'):
        add_up(0, 0, 3, 0, NH, (0,))
    with jax.named_scope('p16_w4'):
        w_wave(4)
    with jax.named_scope('p16_rem3b'):
        add_up(0, 0, 3, 0, NH, (1,))
        for s in range(3):
            pb_send(s, 512, NH)
        pb_send(0, 0, 512)
    with jax.named_scope('p16_o0'):
        o_over([(0, 0, (0, 1))], 0, 2)
        o_over(own, 2, 4)
        o_over([(0, 0, (2, 3))], 0, 1, True)
    with jax.named_scope('p16_w5'):
        w_wave(5)
    with jax.named_scope('p17_x2'):
        for h in (0, 1):
            x_recv(2, h)
    with jax.named_scope('p17_rem1'):
        add_up(0, 3, 4, 512, NH)
        pb_send(3, 512, NH)
        for s in (1, 2):
            pb_send(s, 0, 512)
    with jax.named_scope('p18_w6'):
        w_wave(6)
    with jax.named_scope('p18_rem1q'):
        add_up(0, 3, 4, 0, 512)
        pb_send(3, 0, 512)
    with jax.named_scope('p18_wdone'):
        w_arrived(0)
        w_arrived(1)
    with jax.named_scope('p19_kv'):
        add_up(1, 0, 4, 512, NH)
    with jax.named_scope('p20_rbkv'):
        rb_recv(512, NH)

    kv_cps = []

    def total(i, b, lo, hi):
        off = (i + 4 - x) % 4
        slot = off + (off // 2) * (1 - 2 * (off % 2))
        t = acc[pl.ds(pl.multiple_of(slot * BLK, BLK), BLK), b * NH + lo : b * NH + hi]
        return (t + RB[b, i, :, lo:hi].astype(jnp.float32)).astype(jnp.bfloat16)

    with jax.named_scope('p20_keepkv'):
        for i in range(4):
            ref = KV.at[2 * i + yh]
            ref[:, 0:HD] = total(i, 0, 512, NH)
            ref[:, HD:NKV] = total(i, 1, 512, NH)
            cp = pltpu.make_async_remote_copy(
                ref, ref, kvs.at[i], kvr.at[i], device_id=pair, device_id_type=MESH
            )
            cp.start()
            kv_cps.append(cp)
    with jax.named_scope('p20_o'):
        o_over([(3, 0, (0,))], 0, 2)
        o_over([(3, 0, (2, 3)), (1, 0, (2, 3))], 2, 4)
    with jax.named_scope('p21_q'):
        add_up(1, 0, 4, 0, 512)
    with jax.named_scope('p21_rbq'):
        rb_recv(0, 512)
    with jax.named_scope('p21_keepq'):
        for i in range(4):
            Q[i, :, 0:512] = total(i, 0, 0, 512)
            Q[i, :, 512:NQ] = total(i, 1, 0, 512)
    with jax.named_scope('p21_o'):
        o_over([(3, 0, (0,))], 2, 4, True)
        o_over([(0, 0, (2, 3))], 1, 2, True)
        o_over([(3, 0, (2, 3))], 0, 2, True)
        o_over([(1, 0, (2, 3))], 0, 2)
    scale = HD ** (-0.5)

    def h_ref(j, a, u):
        sg = 1 - 2 * a
        return HG.at[j, (x + 4 + sg * u) % 4, 2 * a : 2 * a + 2]

    def h_send(j, a, u, k):
        sg = 1 - 2 * a
        r = 1 if k != 1 else -1
        ref = h_ref(j, a, u)
        pltpu.make_async_remote_copy(
            ref, ref, hs.at[k], hr.at[j, a, (u - r) % 4],
            device_id=at_x(r * sg), device_id_type=MESH,
        ).start()

    def h_recv(j, a, u):
        ref = h_ref(j, a, u)
        pltpu.make_async_remote_copy(
            ref, ref, hs.at[0], hr.at[j, a, u], device_id=sib, device_id_type=MESH
        ).wait_recv()

    def attend(j):
        rows = pl.ds(pl.multiple_of(j * 32, 32), 32)
        for i in range(4):
            nk = (2 * i + 2) * BLK
            if j == 0:
                ref = KV.at[2 * i + 1 - yh]
                pltpu.make_async_remote_copy(
                    ref, ref, kvs.at[i], kvr.at[i], device_id=pair, device_id_type=MESH
                ).wait_recv()
            q = jnp.concatenate(
                [Q[i, rows, h * HD : (h + 1) * HD] for h in range(8)], axis=0
            )
            kk = KV[0 : 2 * i + 2, :, 0:HD].reshape(nk, HD)
            vv = KV[0 : 2 * i + 2, :, HD:NKV].reshape(nk, HD)
            s = lax.dot_general(
                q, kk, (((1,), (1,)), ((), ())), preferred_element_type=jnp.float32
            ) * scale
            qpos = (2 * i + yh) * BLK + j * 32 + lax.broadcasted_iota(
                jnp.int32, (256, nk), 0
            ) % 32
            kpos = lax.broadcasted_iota(jnp.int32, (256, nk), 1)
            s = jnp.where(qpos >= kpos, s, jnp.float32(-1e30))
            e = jnp.exp(s - jnp.max(s, axis=-1, keepdims=True))
            pr = (e * (1.0 / jnp.sum(e, axis=-1, keepdims=True))).astype(jnp.bfloat16)
            o = jnp.dot(pr, vv, preferred_element_type=jnp.float32).astype(jnp.bfloat16)
            for h in range(8):
                HG[j, x, i, :, h * HD : (h + 1) * HD] = o[h * 32 : (h + 1) * 32]
            if i % 2:
                h_send(j, i // 2, 0, 0)
                h_send(j, i // 2, 0, 1)

    def h_forward(j):
        for a in (0, 1):
            h_recv(j, a, 3)
            h_send(j, a, 3, 2)

    with jax.named_scope('p24_attend0'):
        attend(0)
    with jax.named_scope('p24_attend1'):
        attend(1)
    with jax.named_scope('p24a_o3'):
        o_over([(0, 3, (2,)), (2, 0, (2, 3)), (3, 3, (2,))], 2, 4)
    with jax.named_scope('p24b_o4'):
        o_over([(2, 0, (2, 3)), (0, 3, (2,))], 0, 2)
        o_over([(1, 3, (2,))], 2, 4)
    with jax.named_scope('p24c_attend2'):
        attend(2)
    with jax.named_scope('p24d_hf0'):
        h_forward(0)
    with jax.named_scope('p24e_attend3'):
        attend(3)
    with jax.named_scope('p24e_o5'):
        o_over([(2, 3, (2,))], 2, 4)
    with jax.named_scope('p24f_hf1'):
        h_forward(1)
    with jax.named_scope('p24g_o6'):
        o_over([(3, 3, (2,)), (1, 3, (2,))], 0, 2)
    with jax.named_scope('p24g_hf2'):
        h_forward(2)
    with jax.named_scope('p24h_o7'):
        o_over([(2, 3, (2,))], 0, 2)
    with jax.named_scope('p25_o5'):
        o_wave(5)
    with jax.named_scope('p26_odone0'):
        o_arrived(0)

    def out_ref(j, xx):
        return out.at[
            pl.ds(pl.multiple_of(j * 32, 32), 32), pl.ds(pl.multiple_of(xx * NO, NO), NO)
        ]

    order = [(0, 0), (0, 1), (0, 3), (1, 0), (1, 1), (1, 3), (3, 0), (3, 1)]
    order += [(3, 3), (0, 2), (1, 2), (3, 2), (2, 0), (2, 1), (2, 2), (2, 3)]

    def chip_at(q):
        yy, zz = (y + order[q][0]) % 4, (z + order[q][1]) % 4
        return (yy // 2) * 8 + 2 * zz + yy % 2

    def tile(j, n):
        t = jnp.zeros((BLK, 512), jnp.float32)
        for kc in range(8):
            wo = jnp.concatenate(
                [WO[2 * chip_at(4 * n + e) + kc // 4, kc % 4] for e in range(4)], axis=1
            )
            lhs = HG[j, kc // 2, :, :, (kc % 2) * 512 : (kc % 2) * 512 + 512].reshape(BLK, 512)
            t += jnp.dot(lhs, wo, preferred_element_type=jnp.float32)
        OB[j, :, :, n * 512 : (n + 1) * 512] = t.astype(jnp.bfloat16).reshape(4, 32, 512)
        for q in range(4 * n, 4 * n + 4):
            col = pl.multiple_of(x * NO + chip_at(q) * BLK, BLK)
            dst = out.at[pl.ds(pl.multiple_of(j * 32, 32), 32), pl.ds(col, BLK)]
            cols = slice(q * BLK, (q + 1) * BLK)
            for r in (2, 1, 3):
                pltpu.make_async_remote_copy(
                    OB.at[j, (x + r) % 4, :, cols], dst, os_.at[r], or_.at[j, 4 - r],
                    device_id=at_x(r), device_id_type=MESH,
                ).start()
            pltpu.make_async_copy(OB.at[j, x, :, cols], dst, ol).start()

    def early(j, _):
        with jax.named_scope('m_wait'):
            for a in (0, 1):
                h_recv(j, a, 1)
                h_recv(j, a, 2)
        tile(j, 0)
        tile(j, 1)
        return 0

    def late(j, _):
        tile(j, 2)
        tile(j, 3)
        return 0

    with jax.named_scope('p27_mix0'):
        lax.fori_loop(0, 1, early, 0)
    with jax.named_scope('p27_mix0_hf3'):
        h_forward(3)
    with jax.named_scope('p27_mix1'):
        lax.fori_loop(1, 2, early, 0)
    with jax.named_scope('p27_o6'):
        o_wave(6)
    with jax.named_scope('p27_p_mix2'):
        lax.fori_loop(2, 3, early, 0)
    with jax.named_scope('p27_q_odone1'):
        o_arrived(1)
    with jax.named_scope('p27_r_late'):
        lax.fori_loop(0, 2, late, 0)
    with jax.named_scope('p27_s_mix3'):
        lax.fori_loop(3, 4, early, 0)
    with jax.named_scope('p27_t_late'):
        lax.fori_loop(2, 4, late, 0)

    with jax.named_scope('p28_sent'):
        for cp in x_sends + pb_cps + kv_cps:
            cp.wait_send()
        for part in out_rem + out_own:
            part[1].wait_send()
    wo_swap.wait_send()
    r_sent()
    w_sent()
    o_sent()
    for k in range(3):
        pltpu.make_async_remote_copy(
            HG.at[0], HG.at[0], hs.at[k], hs.at[k], device_id=sib, device_id_type=MESH
        ).wait_send()
    for r in (1, 2, 3):
        pltpu.make_async_remote_copy(
            OB.at[0], OB.at[0], os_.at[r], os_.at[r], device_id=sib, device_id_type=MESH
        ).wait_send()
    pltpu.make_async_copy(OB.at[0], OB.at[0], ol).wait()

    def finish(j, _):
        for r in (1, 2, 3):
            d = out_ref(j, (x + r) % 4)
            pltpu.make_async_remote_copy(
                d, d, os_.at[r], or_.at[j, r], device_id=sib, device_id_type=MESH
            ).wait_recv()
        return 0

    with jax.named_scope('p29_finish'):
        lax.fori_loop(0, 4, finish, 0)


def body(tokens, norm_gain, w_query, key_weight, value_weight, w_out):
    hbm = pl.BlockSpec(memory_space=pltpu.HBM)
    vmem = pl.BlockSpec(memory_space=pltpu.VMEM)
    bf = jnp.bfloat16
    dma = pltpu.SemaphoreType.DMA
    branch = pl.pallas_call(
        kernel,
        out_shape=jax.ShapeDtypeStruct((BLK, D), bf),
        in_specs=[hbm, vmem, hbm, hbm, hbm, hbm],
        out_specs=hbm,
        scratch_shapes=[
            pltpu.VMEM((2, 2, 2, 2, 4, 2, 2, 64, NH), bf),
            pltpu.VMEM((32, 4, 512, BLK), bf),
            pltpu.VMEM((BLK, D), bf),
            pltpu.VMEM((2, 4, BLK, 2048), bf),
            pltpu.VMEM((4, BLK, NQ), bf),
            pltpu.VMEM((8, BLK, NKV), bf),
            pltpu.VMEM((4, 4, 4, 32, NQ), bf),
            pltpu.VMEM((4, 4, 32, NO), bf),
            pltpu.VMEM((4 * BLK, NW), jnp.float32),
            pltpu.VMEM((2, 64, 2048), bf),
            pltpu.VMEM((4, 2, BLK, NH), bf),
            pltpu.VMEM((2, 4, BLK, NH), bf),
            dma((12,)), dma((8,)), dma((8,)), dma((4, 2)), dma((4, 2)), dma((4, 2, 2)), dma((2, 4, 2)),
            dma((2, 5)), dma((2, 4, 4, 4)), dma((2, 2)),
            dma((5,)), dma((4, 4, 4)), dma((2,)),
            dma((4,)), dma((4,)), dma((3,)), dma((4, 2, 4)),
            dma((4,)), dma((4, 4)), dma(()),
        ],
        compiler_params=pltpu.CompilerParams(
            collective_id=0, has_side_effects=True, vmem_limit_bytes=60600000
        ),
        name="sublayer",
    )(tokens[0], norm_gain.reshape(1, D), w_query, key_weight, value_weight, w_out.T)
    return tokens.astype(jnp.float32) + branch[None].astype(jnp.float32)


def solution(mesh):
    placed = (
        P("fsdp", "seq", None),
        P(),
        P(("seq", "fsdp"), None),
        P(("seq", "fsdp"), None),
        P(("seq", "fsdp"), None),
        P(None, ("seq", "fsdp")),
    )
    return jax.shard_map(
        body, mesh=mesh, in_specs=placed, out_specs=P("fsdp", "seq", None), check_vma=False
    )
```

```python
import jax
import jax.numpy as jnp
from jax import lax
from jax.experimental import pallas as pl
from jax.experimental.pallas import tpu as pltpu
from jax.sharding import PartitionSpec as P

HD = 128
BLK = 128
D = 8192
NQ = 1024
NKV = 256
NW = NQ + NKV
NO = 2048
MESH = pl.DeviceIdType.MESH
SLOT = (0, 1, 3, 2)
NH = 640


def kernel(
    tok, gain, wq, wk, wv, wot, out,
    W, WO, XN, X, Q, KV, HG, OB, acc,
    T, PB, RB, loc, xs, xr, xss, xrs, pbs, rbr, wS, wR, wRD, oS, oR, oRD, kvs, kvr, hs, hr, os_, or_, ol,
):
    sx = lax.axis_index("seq")
    f = lax.axis_index("fsdp")
    x, yh = sx // 2, sx % 2
    z, yl, c = f // 4, (f // 2) % 2, f % 2
    y = 2 * yh + yl
    p = yh * 16 + f

    def dev(xx, yy, zz, cc):
        return (2 * xx + yy // 2, 4 * zz + 2 * (yy % 2) + cc)

    def at_x(r):
        return dev((x + r) % 4, y, z, c)

    sib = dev(x, y, z, 1 - c)
    pair = dev(x, (y + 2) % 4, z, c)

    barrier = pltpu.get_barrier_semaphore()
    peers = [at_x(1), at_x(2), at_x(3), sib, pair]
    peers += [dev(x, (y + 1) % 4, z, c), dev(x, (y + 3) % 4, z, c)]
    peers += [dev(x, y, (z + 1) % 4, c), dev(x, y, (z + 3) % 4, c)]
    for d in peers:
        pl.semaphore_signal(barrier, inc=1, device_id=d, device_id_type=MESH)

    def w_parts(t, h, make):
        def dst(g, s, lo, hi):
            return W.at[g, h, s, yh, z, yl, c, :, lo:hi]

        def wide(n, half):
            return wq.at[:, pl.ds(pl.multiple_of(n * NQ + half * 512, 512), 512)]

        def narrow(w, n):
            return w.at[:, pl.ds(pl.multiple_of(n * HD, HD), HD)]

        rem, own = [], []
        for m, d in ((0, 1), (1, 3)):
            n = (t + d) % 4
            rem.append((None, make(wide(n, t // 2), dst(0, m, 0, 512), 2 * m)))
            rem.append(
                (
                    t // 2,
                    make(narrow(wk, n), dst(0, m, 512, NH), 2 * m + 1),
                    make(narrow(wv, n), dst(0, m, 512, NH), 2 * m + 1),
                )
            )
        for s, w in ((0, wk), (1, wv)):
            own.append((None, make(wide(t, s), dst(1, s, 0, 512), 4 + 2 * s)))
            own.append((None, make(narrow(w, t), dst(1, s, 512, NH), 5 + 2 * s)))
        return rem, own

    def begin(part):
        if part[0] is None:
            part[1].start()
        else:
            for k in (0, 1):
                pl.when(part[0] == k)(part[1 + k].start)

    def local(s, d, k):
        return pltpu.make_async_copy(s, d, loc.at[4 + k // 4])

    def remote(s, d, k):
        return pltpu.make_async_remote_copy(
            s, d, xs, xr.at[k // 4], device_id=at_x(2), device_id_type=MESH
        )

    in_rem, in_own = w_parts(x, 0, local)
    for part in in_rem + in_own:
        begin(part)
    khalf = pl.ds(pl.multiple_of(c * 2048, 2048), 2048)
    other = pl.ds(pl.multiple_of((1 - c) * 2048, 2048), 2048)
    tok_in = pltpu.make_async_copy(tok, XN, loc.at[0])
    tok_in.start()
    wo_in = pltpu.make_async_copy(wot.at[:, khalf], T.at[c], loc.at[1])
    wo_in.start()

    with jax.named_scope('p01_barrier'):
        pl.semaphore_wait(barrier, len(peers))

    out_rem, out_own = w_parts((x + 2) % 4, 1, remote)
    for part in out_rem + out_own:
        begin(part)
    wo_swap = pltpu.make_async_remote_copy(
        wot.at[:, other], T.at[c], loc.at[2], loc.at[3], device_id=sib, device_id_type=MESH
    )
    wo_swap.start()

    def w_local(g):
        d = W.at[g, 0, :, yh, z, yl, c]
        pltpu.make_async_copy(d, d, loc.at[4 + g]).wait()

    def w_got(g):
        d = W.at[g, 1, :, yh, z, yl, c]
        pltpu.make_async_remote_copy(
            d, d, xs, xr.at[g], device_id=at_x(2), device_id_type=MESH
        ).wait_recv()

    def gather(S, R, RD, piece, many):
        def coords(h, a1, a2):
            g, sg = h // 2, 1 - 2 * (h % 2)
            yy = (y + 4 + sg * (a1 * g + a2 * (1 - g))) % 4
            zz = (z + 4 + sg * (a1 * (1 - g) + a2 * g)) % 4
            return yy, zz

        def ref(h, u1, u2):
            yy, zz = coords(h, u1, u2)
            return piece(h, yy, zz)

        def lane(u1, u2):
            return {0: u1 - 1, 1: 7, 2: 8, 3: 3 + u1}[u2]

        def send(h, u1, u2, k):
            a1, a2 = ((1, 0), (-1, 0), (0, 1), (0, -1))[k]
            yy, zz = coords(h, a1, a2)
            r = ref(h, u1, u2)
            pltpu.make_async_remote_copy(
                r, r, S.at[k], R.at[h, lane((u1 - a1) % 4, (u2 - a2) % 4)],
                device_id=dev(x, yy, zz, c), device_id_type=MESH,
            ).start()

        def across(h, u1, u2):
            r = ref(h, u1, u2)
            pltpu.make_async_remote_copy(
                r, r, S.at[4], RD.at[int(u2 == 2)], device_id=sib, device_id_type=MESH
            ).start()

        def recv(h, u1, u2):
            r = ref(h, u1, u2) if u2 in (0, 3) else many(4)
            pltpu.make_async_remote_copy(
                r, r, S.at[4], R.at[h, lane(u1, u2)], device_id=sib, device_id_type=MESH
            ).wait_recv()

        def over_pieces(steps, first=0, last=4, again=False):
            def one(h, _):
                for u1, u2, ks in steps:
                    if not again and (u1, u2) != (0, 0) and (u2 in (0, 3) or u1 == 0):
                        recv(h, u1, u2)
                    for k in ks:
                        send(h, u1, u2, k)
                    if not again:
                        across(h, u1, u2)
                return 0

            lax.fori_loop(first, last, one, 0)

        def whole(sem, n):
            return pltpu.make_async_remote_copy(
                many(n), many(n), sem, sem, device_id=sib, device_id_type=MESH
            )

        def wave(n):
            if n == 1:
                over_pieces([(3, 0, (0,))])
                over_pieces([(3, 0, (2, 3))], again=True)
                over_pieces([(1, 0, (2, 3))])
            elif n == 2:
                over_pieces([(2, 0, (2, 3)), (0, 3, (2,))])
            elif n == 3:
                over_pieces([(3, 3, (2,)), (1, 3, (2,))])
            elif n == 4:
                over_pieces([(2, 3, (2,))])
            elif n == 5:
                over_pieces([(u, 1, ()) for u in (0, 3, 1, 2)])
            elif n == 6:
                over_pieces([(u, 2, ()) for u in (0, 3, 1, 2)])

        def arrived(k):
            whole(RD.at[k], (48, 16)[k]).wait_recv()

        def sent():
            for k, n in enumerate((8, 4, 32, 16, 64)):
                whole(S.at[k], n).wait_send()

        return over_pieces, wave, arrived, sent

    def w_many(n):
        if n == 64:
            return W.at[0, 0]
        if n == 48:
            return W.at[0, 0, :, :, 0:3]
        if n == 32:
            return W.at[0, 0, 0]
        if n == 16:
            return W.at[0, 0, 0, 0]
        return W.at[0, 0, 0, 0, 0 : n // 4]

    def w_gather(g):
        return gather(
            wS.at[g], wR.at[g], wRD.at[g],
            lambda e, yy, zz: W.at[g, e % 2, e // 2, yy // 2, zz, yy % 2, c],
            w_many,
        )

    r_over, r_wave, r_arrived, r_sent = w_gather(0)
    w_over, w_wave, w_arrived, w_sent = w_gather(1)
    o_over, o_wave, o_arrived, o_sent = gather(
        oS, oR, oRD,
        lambda e, yy, zz: WO.at[(yy // 2) * 16 + 4 * zz + 2 * (yy % 2) + c, e],
        lambda n: WO.at[0 : n // 4],
    )

    own = [(0, 0, (0, 1, 2, 3))]

    def each(over, steps, pieces):
        for e in pieces:
            over(steps, e, e + 1)

    with jax.named_scope('p02_r0a'):
        w_local(0)
        each(r_over, own, (0, 2))

    with jax.named_scope('p02_tok'):
        tok_in.wait()

    def norm(r, _):
        rows = pl.ds(pl.multiple_of(r * 16, 16), 16)
        v = XN[rows, :].astype(jnp.float32)
        ms = jnp.mean(v * v, axis=-1, keepdims=True)
        XN[rows, :] = (v * lax.rsqrt(ms + 1e-05) * gain[...]).astype(jnp.bfloat16)
        return 0

    with jax.named_scope('p03_norm'):
        lax.fori_loop(0, BLK // 16, norm, 0)

    def x_cols(ch):
        return pl.ds(pl.multiple_of((ch % 4) * 2048, 2048), 2048)

    def x_copy(r, h):
        o = (4 - r) % 4
        return pltpu.make_async_remote_copy(
            XN.at[:, x_cols(x + r + 2 * h)], X.at[h, SLOT[o]], xss, xrs.at[int(o == 2)],
            device_id=at_x(r), device_id_type=MESH,
        )

    def x_wait(d, k):
        return pltpu.make_async_remote_copy(
            d, d, xss, xrs.at[k], device_id=sib, device_id_type=MESH
        )

    x_sends = [x_copy(r, h) for rs in ((1, 3), (2,)) for h in (0, 1) for r in rs]
    for cp in x_sends:
        cp.start()
    for h in (0, 1):
        X[h, 0] = XN[:, x_cols(x + 2 * h)]

    with jax.named_scope('p04_swap'):
        wo_in.wait()
        wo_swap.wait_recv()
        t = T[...].reshape(BLK, 2048)
        for h in range(4):
            WO[p, h] = t[:, 512 * h : 512 * (h + 1)].T

    with jax.named_scope('p05_w0a'):
        w_local(1)
        each(w_over, own, (0, 2))
    with jax.named_scope('p06_r0b'):
        w_got(0)
        each(r_over, own, (1, 3))
    with jax.named_scope('p07_r1'):
        r_wave(1)
    with jax.named_scope('p08_w0b'):
        w_got(1)
        each(w_over, own, (1, 3))
    with jax.named_scope('p09_r2'):
        r_wave(2)
    with jax.named_scope('p10_r3'):
        r_wave(3)
    with jax.named_scope('p11_r4'):
        r_wave(4)
    with jax.named_scope('p12_w1'):
        w_wave(1)
    with jax.named_scope('p13_r56'):
        r_wave(5)
        r_wave(6)
    with jax.named_scope('p14_w2'):
        w_wave(2)
    with jax.named_scope('p14_w3'):
        w_wave(3)
    with jax.named_scope('p15_rdone'):
        r_arrived(0)
        r_arrived(1)
    with jax.named_scope('p15_x1'):
        x_wait(X.at[:, 1:3], 0).wait_recv()

    def add_up(g, lo, hi, n0, n1, chunks=(0, 1)):
        rows = slice(lo * BLK, hi * BLK)
        n = n1 - n0
        for h in chunks:
            wkc = jnp.concatenate(
                [W[g, h, t, :, :, :, :, :, n0:n1].reshape(2048, n) for t in (0, 1)], axis=1
            )
            d = jnp.dot(
                X[h, lo:hi].reshape((hi - lo) * BLK, 2048), wkc,
                preferred_element_type=jnp.float32,
            )
            for t in (0, 1):
                cols = slice(t * NH + n0, t * NH + n1)
                part = d[:, t * n : (t + 1) * n]
                if h == 0:
                    acc[rows, cols] = part
                else:
                    acc[rows, cols] += part

    def pb_send(s, n0, n1):
        i = (x + SLOT.index(s)) % 4
        for m, r in ((0, 1), (1, 3)):
            PB[s, m, :, n0:n1] = acc[
                s * BLK : (s + 1) * BLK, m * NH + n0 : m * NH + n1
            ].astype(jnp.bfloat16)
            cp = pltpu.make_async_remote_copy(
                PB.at[s, m, :, n0:n1], RB.at[x // 2, i, :, n0:n1],
                pbs.at[n0 // 512], rbr.at[n0 // 512],
                device_id=at_x(r), device_id_type=MESH,
            )
            cp.start()

    def partial(ref, n0, n1):
        ref = ref.at[:, :, :, n0:n1]
        return pltpu.make_async_remote_copy(
            ref, ref, pbs.at[n0 // 512], rbr.at[n0 // 512], device_id=sib, device_id_type=MESH
        )

    with jax.named_scope('p16_rem3a'):
        add_up(0, 0, 3, 0, NH, (0,))
    with jax.named_scope('p16_w4'):
        w_wave(4)
    with jax.named_scope('p16_rem3b'):
        add_up(0, 0, 3, 0, NH, (1,))
        for s in range(3):
            pb_send(s, 512, NH)
        pb_send(0, 0, 512)
    with jax.named_scope('p16_o0'):
        o_over([(0, 0, (0, 1))], 0, 2)
        o_over(own, 2, 4)
        o_over([(0, 0, (2, 3))], 0, 1, True)
    with jax.named_scope('p16_w5'):
        w_wave(5)
    with jax.named_scope('p17_x2'):
        x_wait(X.at[:, 3], 1).wait_recv()
    with jax.named_scope('p17_rem1'):
        add_up(0, 3, 4, 512, NH)
        pb_send(3, 512, NH)
        for s in (1, 2):
            pb_send(s, 0, 512)
    with jax.named_scope('p18_w6'):
        w_wave(6)
    with jax.named_scope('p18_rem1q'):
        add_up(0, 3, 4, 0, 512)
        pb_send(3, 0, 512)
    with jax.named_scope('p18_wdone'):
        w_arrived(0)
        w_arrived(1)
    with jax.named_scope('p19_kv'):
        add_up(1, 0, 4, 512, NH)
    with jax.named_scope('p20_rbkv'):
        partial(RB, 512, NH).wait_recv()

    def total(i, b, lo, hi):
        off = (i + 4 - x) % 4
        slot = off + (off // 2) * (1 - 2 * (off % 2))
        t = acc[pl.ds(pl.multiple_of(slot * BLK, BLK), BLK), b * NH + lo : b * NH + hi]
        return (t + RB[b, i, :, lo:hi].astype(jnp.float32)).astype(jnp.bfloat16)

    with jax.named_scope('p20_keepkv'):
        for i in range(4):
            ref = KV.at[2 * i + yh]
            ref[:, 0:HD] = total(i, 0, 512, NH)
            ref[:, HD:NKV] = total(i, 1, 512, NH)
            cp = pltpu.make_async_remote_copy(
                ref, ref, kvs, kvr.at[i], device_id=pair, device_id_type=MESH
            )
            cp.start()
    with jax.named_scope('p20_o'):
        o_over([(3, 0, (0,))], 0, 2)
        o_over([(3, 0, (2, 3)), (1, 0, (2, 3))], 2, 4)
    with jax.named_scope('p21_q'):
        add_up(1, 0, 4, 0, 512)
    with jax.named_scope('p21_rbq'):
        partial(RB, 0, 512).wait_recv()
    with jax.named_scope('p21_keepq'):
        for i in range(4):
            Q[i, :, 0:512] = total(i, 0, 0, 512)
            Q[i, :, 512:NQ] = total(i, 1, 0, 512)
    with jax.named_scope('p21_o'):
        o_over([(3, 0, (0,))], 2, 4, True)
        o_over([(0, 0, (2, 3))], 1, 2, True)
        o_over([(3, 0, (2, 3))], 0, 2, True)
        o_over([(1, 0, (2, 3))], 0, 2)
    scale = HD ** (-0.5)

    def h_ref(j, a, u):
        sg = 1 - 2 * a
        return HG.at[j, (x + 4 + sg * u) % 4, 2 * a : 2 * a + 2]

    def h_send(j, a, u, k):
        sg = 1 - 2 * a
        r = 1 if k != 1 else -1
        ref = h_ref(j, a, u)
        pltpu.make_async_remote_copy(
            ref, ref, hs.at[k], hr.at[j, a if (u - r) % 4 == 3 else 2],
            device_id=at_x(r * sg), device_id_type=MESH,
        ).start()

    def h_wait(ref, j, k):
        pltpu.make_async_remote_copy(
            ref, ref, hs.at[0], hr.at[j, k], device_id=sib, device_id_type=MESH
        ).wait_recv()

    def attend(j):
        rows = pl.ds(pl.multiple_of(j * 32, 32), 32)
        for i in range(4):
            nk = (2 * i + 2) * BLK
            if j == 0:
                ref = KV.at[2 * i + 1 - yh]
                pltpu.make_async_remote_copy(
                    ref, ref, kvs, kvr.at[i], device_id=pair, device_id_type=MESH
                ).wait_recv()
            q = jnp.concatenate(
                [Q[i, rows, h * HD : (h + 1) * HD] for h in range(8)], axis=0
            )
            kk = KV[0 : 2 * i + 2, :, 0:HD].reshape(nk, HD)
            vv = KV[0 : 2 * i + 2, :, HD:NKV].reshape(nk, HD)
            s = lax.dot_general(
                q, kk, (((1,), (1,)), ((), ())), preferred_element_type=jnp.float32
            ) * scale
            qpos = (2 * i + yh) * BLK + j * 32 + lax.broadcasted_iota(
                jnp.int32, (256, nk), 0
            ) % 32
            kpos = lax.broadcasted_iota(jnp.int32, (256, nk), 1)
            s = jnp.where(qpos >= kpos, s, jnp.float32(-1e30))
            e = jnp.exp(s - jnp.max(s, axis=-1, keepdims=True))
            pr = (e * (1.0 / jnp.sum(e, axis=-1, keepdims=True))).astype(jnp.bfloat16)
            o = jnp.dot(pr, vv, preferred_element_type=jnp.float32).astype(jnp.bfloat16)
            for h in range(8):
                HG[j, x, i, :, h * HD : (h + 1) * HD] = o[h * 32 : (h + 1) * 32]
            if i % 2:
                h_send(j, i // 2, 0, 0)
                h_send(j, i // 2, 0, 1)

    def h_forward(j):
        for a in (0, 1):
            h_wait(h_ref(j, a, 3), j, a)
            h_send(j, a, 3, 2)

    with jax.named_scope('p24_attend0'):
        attend(0)
    with jax.named_scope('p24_attend1'):
        attend(1)
    with jax.named_scope('p24_attend2'):
        attend(2)
    with jax.named_scope('p24a_o3'):
        o_over([(0, 3, (2,)), (2, 0, (2, 3)), (3, 3, (2,))], 2, 4)
    with jax.named_scope('p24d_hf0'):
        h_forward(0)
    with jax.named_scope('p24d_o4'):
        o_over([(2, 0, (2, 3)), (0, 3, (2,))], 0, 2)
        o_over([(1, 3, (2,))], 2, 4)
    with jax.named_scope('p24e_attend3'):
        attend(3)
    with jax.named_scope('p24e_o5'):
        o_over([(2, 3, (2,))], 2, 4)
    with jax.named_scope('p24f_hf1'):
        h_forward(1)
    with jax.named_scope('p24g_o6'):
        o_over([(3, 3, (2,)), (1, 3, (2,))], 0, 2)
    with jax.named_scope('p24g_hf2'):
        h_forward(2)
    with jax.named_scope('p24h_o7'):
        o_over([(2, 3, (2,))], 0, 2)
    with jax.named_scope('p25_o5'):
        o_wave(5)
    with jax.named_scope('p26_odone0'):
        o_arrived(0)

    def out_ref(j, xx):
        return out.at[
            pl.ds(pl.multiple_of(j * 32, 32), 32), pl.ds(pl.multiple_of(xx * NO, NO), NO)
        ]

    order = [(0, 0), (0, 1), (0, 3), (1, 0), (1, 1), (1, 3), (3, 0), (3, 1)]
    order += [(3, 3), (0, 2), (1, 2), (3, 2), (2, 0), (2, 1), (2, 2), (2, 3)]

    def chip_at(q):
        yy, zz = (y + order[q][0]) % 4, (z + order[q][1]) % 4
        return (yy // 2) * 8 + 2 * zz + yy % 2

    def tile(j, n):
        t = jnp.zeros((BLK, 512), jnp.float32)
        for kc in range(8):
            wo = jnp.concatenate(
                [WO[2 * chip_at(4 * n + e) + kc // 4, kc % 4] for e in range(4)], axis=1
            )
            lhs = HG[j, kc // 2, :, :, (kc % 2) * 512 : (kc % 2) * 512 + 512].reshape(BLK, 512)
            t += jnp.dot(lhs, wo, preferred_element_type=jnp.float32)
        OB[j, :, :, n * 512 : (n + 1) * 512] = t.astype(jnp.bfloat16).reshape(4, 32, 512)
        for q in range(4 * n, 4 * n + 4):
            col = pl.multiple_of(x * NO + chip_at(q) * BLK, BLK)
            dst = out.at[pl.ds(pl.multiple_of(j * 32, 32), 32), pl.ds(col, BLK)]
            cols = slice(q * BLK, (q + 1) * BLK)
            for r in (2, 1, 3):
                pltpu.make_async_remote_copy(
                    OB.at[j, (x + r) % 4, :, cols], dst, os_.at[r - 1], or_.at[3 - r],
                    device_id=at_x(r), device_id_type=MESH,
                ).start()
            pltpu.make_async_copy(OB.at[j, x, :, cols], dst, ol).start()

    def early(j, _):
        with jax.named_scope('m_wait'):
            h_wait(HG.at[j, 0:2], j, 2)
        tile(j, 0)
        tile(j, 1)
        return 0

    def late(j, _):
        tile(j, 2)
        tile(j, 3)
        return 0

    with jax.named_scope('p27_mix0'):
        lax.fori_loop(0, 1, early, 0)
    with jax.named_scope('p27_mix0_hf3'):
        h_forward(3)
    with jax.named_scope('p27_mix1'):
        lax.fori_loop(1, 2, early, 0)
    with jax.named_scope('p27_o6'):
        o_wave(6)
    with jax.named_scope('p27_p_mix2'):
        lax.fori_loop(2, 3, early, 0)
    with jax.named_scope('p27_q_odone1'):
        o_arrived(1)
    with jax.named_scope('p27_r_late'):
        lax.fori_loop(0, 2, late, 0)
    with jax.named_scope('p27_s_mix3'):
        lax.fori_loop(3, 4, early, 0)
    with jax.named_scope('p27_t_late'):
        lax.fori_loop(2, 4, late, 0)

    with jax.named_scope('p28_sent'):
        x_wait(X.at[:, 0:3], 0).wait_send()
        for n0, n1 in ((512, NH), (0, 512)):
            partial(PB, n0, n1).wait_send()
        d = KV.at[0:4]
        pltpu.make_async_remote_copy(
            d, d, kvs, kvr.at[0], device_id=pair, device_id_type=MESH
        ).wait_send()
        d = W.at[:, 0, :, 0, 0, 0, 0]
        pltpu.make_async_remote_copy(
            d, d, xs, xr.at[0], device_id=at_x(2), device_id_type=MESH
        ).wait_send()
        wo_swap.wait_send()
        r_sent()
        w_sent()
        o_sent()
        for k in range(3):
            pltpu.make_async_remote_copy(
                HG.at[0], HG.at[0], hs.at[k], hr.at[0, 0], device_id=sib, device_id_type=MESH
            ).wait_send()
    with jax.named_scope('p29_finish'):
        for r in (1, 2, 3):
            pltpu.make_async_remote_copy(
                OB.at[0], OB.at[0], os_.at[r - 1], or_.at[r - 1],
                device_id=sib, device_id_type=MESH,
            ).wait()
        pltpu.make_async_copy(OB.at[0], OB.at[0], ol).wait()


def body(tokens, norm_gain, w_query, key_weight, value_weight, w_out):
    hbm = pl.BlockSpec(memory_space=pltpu.HBM)
    vmem = pl.BlockSpec(memory_space=pltpu.VMEM)
    bf = jnp.bfloat16
    dma = pltpu.SemaphoreType.DMA
    branch = pl.pallas_call(
        kernel,
        out_shape=jax.ShapeDtypeStruct((BLK, D), bf),
        in_specs=[hbm, vmem, hbm, hbm, hbm, hbm],
        out_specs=hbm,
        scratch_shapes=[
            pltpu.VMEM((2, 2, 2, 2, 4, 2, 2, 64, NH), bf),
            pltpu.VMEM((32, 4, 512, BLK), bf),
            pltpu.VMEM((BLK, D), bf),
            pltpu.VMEM((2, 4, BLK, 2048), bf),
            pltpu.VMEM((4, BLK, NQ), bf),
            pltpu.VMEM((8, BLK, NKV), bf),
            pltpu.VMEM((4, 4, 4, 32, NQ), bf),
            pltpu.VMEM((4, 4, 32, NO), bf),
            pltpu.VMEM((4 * BLK, NW), jnp.float32),
            pltpu.VMEM((2, 64, 2048), bf),
            pltpu.VMEM((4, 2, BLK, NH), bf),
            pltpu.VMEM((2, 4, BLK, NH), bf),
            dma((6,)), dma(()), dma((2,)), dma(()), dma((2,)), dma((2,)), dma((2,)),
            dma((2, 5)), dma((2, 4, 9)), dma((2, 2)),
            dma((5,)), dma((4, 9)), dma((2,)),
            dma(()), dma((4,)), dma((3,)), dma((4, 3)),
            dma((3,)), dma((3,)), dma(()),
        ],
        compiler_params=pltpu.CompilerParams(
            collective_id=0, has_side_effects=True, vmem_limit_bytes=60600000
        ),
        name="sublayer",
    )(tokens[0], norm_gain.reshape(1, D), w_query, key_weight, value_weight, w_out.T)
    return tokens.astype(jnp.float32) + branch[None].astype(jnp.float32)


def solution(mesh):
    placed = (
        P("fsdp", "seq", None),
        P(),
        P(("seq", "fsdp"), None),
        P(("seq", "fsdp"), None),
        P(("seq", "fsdp"), None),
        P(None, ("seq", "fsdp")),
    )
    return jax.shard_map(
        body, mesh=mesh, in_specs=placed, out_specs=P("fsdp", "seq", None), check_vma=False
    )
```

```python
import jax
import jax.numpy as jnp
from jax import lax
from jax.experimental import pallas as pl
from jax.experimental.pallas import tpu as pltpu
from jax.sharding import PartitionSpec as P

HD = 128
BLK = 128
D = 8192
NQ = 1024
NKV = 256
NW = NQ + NKV
NO = 2048
MESH = pl.DeviceIdType.MESH
SLOT = (0, 1, 3, 2)
NH = 640


def kernel(
    tok, gain, wq, wk, wv, wot, out,
    W, WO, XN, X, Q, KV, HG, OB, acc,
    T, PB, RB, loc, xs, xr, xss, xrs, pbs, rbr, wS, wR, wRD, oS, oR, oRD, kvs, kvr, hs, hr, os_, or_, ol,
):
    sx = lax.axis_index("seq")
    f = lax.axis_index("fsdp")
    x, yh = sx // 2, sx % 2
    z, yl, c = f // 4, (f // 2) % 2, f % 2
    y = 2 * yh + yl
    p = yh * 16 + f

    def dev(xx, yy, zz, cc):
        return (2 * xx + yy // 2, 4 * zz + 2 * (yy % 2) + cc)

    def at_x(r):
        return dev((x + r) % 4, y, z, c)

    sib = dev(x, y, z, 1 - c)
    pair = dev(x, (y + 2) % 4, z, c)

    barrier = pltpu.get_barrier_semaphore()
    peers = [at_x(1), at_x(2), at_x(3), sib, pair]
    peers += [dev(x, (y + 1) % 4, z, c), dev(x, (y + 3) % 4, z, c)]
    peers += [dev(x, y, (z + 1) % 4, c), dev(x, y, (z + 3) % 4, c)]
    for d in peers:
        pl.semaphore_signal(barrier, inc=1, device_id=d, device_id_type=MESH)

    def w_parts(t, h, make):
        def dst(g, s, lo, hi):
            return W.at[g, h, s, yh, z, yl, c, :, lo:hi]

        def wide(n, half):
            return wq.at[:, pl.ds(pl.multiple_of(n * NQ + half * 512, 512), 512)]

        def narrow(w, n):
            return w.at[:, pl.ds(pl.multiple_of(n * HD, HD), HD)]

        rem, own = [], []
        for m, d in ((0, 1), (1, 3)):
            n = (t + d) % 4
            rem.append((None, make(wide(n, t // 2), dst(0, m, 0, 512), 2 * m)))
            rem.append(
                (
                    t // 2,
                    make(narrow(wk, n), dst(0, m, 512, NH), 2 * m + 1),
                    make(narrow(wv, n), dst(0, m, 512, NH), 2 * m + 1),
                )
            )
        for s, w in ((0, wk), (1, wv)):
            own.append((None, make(wide(t, s), dst(1, s, 0, 512), 4 + 2 * s)))
            own.append((None, make(narrow(w, t), dst(1, s, 512, NH), 5 + 2 * s)))
        return rem, own

    def begin(part):
        if part[0] is None:
            part[1].start()
        else:
            for k in (0, 1):
                pl.when(part[0] == k)(part[1 + k].start)

    def local(s, d, k):
        return pltpu.make_async_copy(s, d, loc.at[4 + k // 4])

    def remote(s, d, k):
        return pltpu.make_async_remote_copy(
            s, d, xs, xr.at[k // 4], device_id=at_x(2), device_id_type=MESH
        )

    in_rem, in_own = w_parts(x, 0, local)
    for part in in_rem + in_own:
        begin(part)
    khalf = pl.ds(pl.multiple_of(c * 2048, 2048), 2048)
    other = pl.ds(pl.multiple_of((1 - c) * 2048, 2048), 2048)
    tok_in = pltpu.make_async_copy(tok, XN, loc.at[0])
    tok_in.start()
    wo_in = pltpu.make_async_copy(wot.at[:, khalf], T.at[c], loc.at[1])
    wo_in.start()

    with jax.named_scope('p01_barrier'):
        pl.semaphore_wait(barrier, len(peers))

    out_rem, out_own = w_parts((x + 2) % 4, 1, remote)
    for part in out_rem + out_own:
        begin(part)
    wo_swap = pltpu.make_async_remote_copy(
        wot.at[:, other], T.at[c], loc.at[2], loc.at[3], device_id=sib, device_id_type=MESH
    )
    wo_swap.start()

    def w_local(g):
        d = W.at[g, 0, :, yh, z, yl, c]
        pltpu.make_async_copy(d, d, loc.at[4 + g]).wait()

    def w_got(g):
        d = W.at[g, 1, :, yh, z, yl, c]
        pltpu.make_async_remote_copy(
            d, d, xs, xr.at[g], device_id=at_x(2), device_id_type=MESH
        ).wait_recv()

    def gather(S, R, RD, piece, many):
        def coords(h, a1, a2):
            g, sg = h // 2, 1 - 2 * (h % 2)
            yy = (y + 4 + sg * (a1 * g + a2 * (1 - g))) % 4
            zz = (z + 4 + sg * (a1 * (1 - g) + a2 * g)) % 4
            return yy, zz

        def ref(h, u1, u2):
            yy, zz = coords(h, u1, u2)
            return piece(h, yy, zz)

        def lane(u1, u2):
            return {0: u1 - 1, 1: 7, 2: 8, 3: 3 + u1}[u2]

        def send(h, u1, u2, k):
            a1, a2 = ((1, 0), (-1, 0), (0, 1), (0, -1))[k]
            yy, zz = coords(h, a1, a2)
            r = ref(h, u1, u2)
            pltpu.make_async_remote_copy(
                r, r, S.at[k], R.at[h, lane((u1 - a1) % 4, (u2 - a2) % 4)],
                device_id=dev(x, yy, zz, c), device_id_type=MESH,
            ).start()

        def across(h, u1, u2):
            r = ref(h, u1, u2)
            pltpu.make_async_remote_copy(
                r, r, S.at[4], RD.at[int(u2 == 2)], device_id=sib, device_id_type=MESH
            ).start()

        def recv(h, u1, u2):
            r = ref(h, u1, u2) if u2 in (0, 3) else many(4)
            pltpu.make_async_remote_copy(
                r, r, S.at[4], R.at[h, lane(u1, u2)], device_id=sib, device_id_type=MESH
            ).wait_recv()

        def over_pieces(steps, first=0, last=4, again=False):
            def one(h, _):
                for u1, u2, ks in steps:
                    if not again and (u1, u2) != (0, 0) and (u2 in (0, 3) or u1 == 0):
                        recv(h, u1, u2)
                    for k in ks:
                        send(h, u1, u2, k)
                    if not again:
                        across(h, u1, u2)
                return 0

            lax.fori_loop(first, last, one, 0)

        def whole(sem, n):
            return pltpu.make_async_remote_copy(
                many(n), many(n), sem, sem, device_id=sib, device_id_type=MESH
            )

        def wave(n):
            if n == 1:
                over_pieces([(3, 0, (0,))])
                over_pieces([(3, 0, (2, 3))], again=True)
                over_pieces([(1, 0, (2, 3))])
            elif n == 2:
                over_pieces([(2, 0, (2, 3)), (0, 3, (2,))])
            elif n == 3:
                over_pieces([(3, 3, (2,)), (1, 3, (2,))])
            elif n == 4:
                over_pieces([(2, 3, (2,))])
            elif n == 5:
                over_pieces([(u, 1, ()) for u in (0, 3, 1, 2)])
            elif n == 6:
                over_pieces([(u, 2, ()) for u in (0, 3, 1, 2)])

        def arrived(k):
            whole(RD.at[k], (48, 16)[k]).wait_recv()

        def sent():
            for k, n in enumerate((8, 4, 32, 16, 64)):
                whole(S.at[k], n).wait_send()

        return over_pieces, wave, arrived, sent

    def w_many(n):
        if n == 64:
            return W.at[0, 0]
        if n == 48:
            return W.at[0, 0, :, :, 0:3]
        if n == 32:
            return W.at[0, 0, 0]
        if n == 16:
            return W.at[0, 0, 0, 0]
        return W.at[0, 0, 0, 0, 0 : n // 4]

    def w_gather(g):
        return gather(
            wS.at[g], wR.at[g], wRD.at[g],
            lambda e, yy, zz: W.at[g, e % 2, e // 2, yy // 2, zz, yy % 2, c],
            w_many,
        )

    r_over, r_wave, r_arrived, r_sent = w_gather(0)
    w_over, w_wave, w_arrived, w_sent = w_gather(1)
    o_over, o_wave, o_arrived, o_sent = gather(
        oS, oR, oRD,
        lambda e, yy, zz: WO.at[(yy // 2) * 16 + 4 * zz + 2 * (yy % 2) + c, e],
        lambda n: WO.at[0 : n // 4],
    )

    own = [(0, 0, (0, 1, 2, 3))]

    def each(over, steps, pieces):
        for e in pieces:
            over(steps, e, e + 1)

    with jax.named_scope('p02_r0a'):
        w_local(0)
        each(r_over, own, (0, 2))

    with jax.named_scope('p02_tok'):
        tok_in.wait()

    def norm(r, _):
        rows = pl.ds(pl.multiple_of(r * 16, 16), 16)
        v = XN[rows, :].astype(jnp.float32)
        ms = jnp.mean(v * v, axis=-1, keepdims=True)
        XN[rows, :] = (v * lax.rsqrt(ms + 1e-05) * gain[...]).astype(jnp.bfloat16)
        return 0

    with jax.named_scope('p03_norm'):
        lax.fori_loop(0, BLK // 16, norm, 0)

    def x_cols(ch):
        return pl.ds(pl.multiple_of((ch % 4) * 2048, 2048), 2048)

    def x_copy(r, h):
        o = (4 - r) % 4
        return pltpu.make_async_remote_copy(
            XN.at[:, x_cols(x + r + 2 * h)], X.at[h, SLOT[o]], xss, xrs.at[int(o == 2)],
            device_id=at_x(r), device_id_type=MESH,
        )

    def x_wait(d, k):
        return pltpu.make_async_remote_copy(
            d, d, xss, xrs.at[k], device_id=sib, device_id_type=MESH
        )

    x_sends = [x_copy(r, h) for rs in ((1, 3), (2,)) for h in (0, 1) for r in rs]
    for cp in x_sends:
        cp.start()
    for h in (0, 1):
        X[h, 0] = XN[:, x_cols(x + 2 * h)]

    with jax.named_scope('p04_swap'):
        wo_in.wait()
        wo_swap.wait_recv()
        t = T[...].reshape(BLK, 2048)
        for h in range(4):
            WO[p, h] = t[:, 512 * h : 512 * (h + 1)].T

    with jax.named_scope('p05_w0a'):
        w_local(1)
        each(w_over, own, (0, 2))
    with jax.named_scope('p06_r0b'):
        w_got(0)
        each(r_over, own, (1, 3))
    with jax.named_scope('p07_r1'):
        r_wave(1)
    with jax.named_scope('p08_w0b'):
        w_got(1)
        each(w_over, own, (1, 3))
    with jax.named_scope('p09_r2'):
        r_wave(2)
    with jax.named_scope('p10_r3'):
        r_wave(3)
    with jax.named_scope('p11_r4'):
        r_wave(4)
    with jax.named_scope('p12_w1'):
        w_wave(1)
    with jax.named_scope('p13_r56'):
        r_wave(5)
        r_wave(6)
    with jax.named_scope('p14_w2'):
        w_wave(2)
    with jax.named_scope('p14_w3'):
        w_wave(3)
    with jax.named_scope('p15_rdone'):
        r_arrived(0)
        r_arrived(1)
    with jax.named_scope('p15_x1'):
        x_wait(X.at[:, 1:3], 0).wait_recv()

    def add_up(g, lo, hi, n0, n1, chunks=(0, 1)):
        rows = slice(lo * BLK, hi * BLK)
        n = n1 - n0
        for h in chunks:
            wkc = jnp.concatenate(
                [W[g, h, t, :, :, :, :, :, n0:n1].reshape(2048, n) for t in (0, 1)], axis=1
            )
            d = jnp.dot(
                X[h, lo:hi].reshape((hi - lo) * BLK, 2048), wkc,
                preferred_element_type=jnp.float32,
            )
            for t in (0, 1):
                cols = slice(t * NH + n0, t * NH + n1)
                part = d[:, t * n : (t + 1) * n]
                if h == 0:
                    acc[rows, cols] = part
                else:
                    acc[rows, cols] += part

    def pb_send(s, n0, n1):
        i = (x + SLOT.index(s)) % 4
        for m, r in ((0, 1), (1, 3)):
            PB[s, m, :, n0:n1] = acc[
                s * BLK : (s + 1) * BLK, m * NH + n0 : m * NH + n1
            ].astype(jnp.bfloat16)
            cp = pltpu.make_async_remote_copy(
                PB.at[s, m, :, n0:n1], RB.at[x // 2, i, :, n0:n1],
                pbs.at[n0 // 512], rbr.at[n0 // 512],
                device_id=at_x(r), device_id_type=MESH,
            )
            cp.start()

    def partial(ref, n0, n1):
        ref = ref.at[:, :, :, n0:n1]
        return pltpu.make_async_remote_copy(
            ref, ref, pbs.at[n0 // 512], rbr.at[n0 // 512], device_id=sib, device_id_type=MESH
        )

    with jax.named_scope('p16_rem3a'):
        add_up(0, 0, 3, 0, NH, (0,))
    with jax.named_scope('p16_w4'):
        w_wave(4)
    with jax.named_scope('p16_rem3b'):
        add_up(0, 0, 3, 0, NH, (1,))
        for s in range(3):
            pb_send(s, 512, NH)
        pb_send(0, 0, 512)
    with jax.named_scope('p16_o0'):
        o_over([(0, 0, (0, 1))], 0, 2)
        o_over(own, 2, 4)
        o_over([(0, 0, (2, 3))], 0, 1, True)
    with jax.named_scope('p16_w5'):
        w_wave(5)
    with jax.named_scope('p17_x2'):
        x_wait(X.at[:, 3], 1).wait_recv()
    with jax.named_scope('p17_rem1'):
        add_up(0, 3, 4, 512, NH)
        pb_send(3, 512, NH)
        for s in (1, 2):
            pb_send(s, 0, 512)
    with jax.named_scope('p18_w6'):
        w_wave(6)
    with jax.named_scope('p18_rem1q'):
        add_up(0, 3, 4, 0, 512)
        pb_send(3, 0, 512)
    with jax.named_scope('p18_wdone'):
        w_arrived(0)
        w_arrived(1)
    with jax.named_scope('p19_kv'):
        add_up(1, 0, 4, 512, NH)
    with jax.named_scope('p20_rbkv'):
        partial(RB, 512, NH).wait_recv()

    def total(i, b, lo, hi):
        off = (i + 4 - x) % 4
        slot = off + (off // 2) * (1 - 2 * (off % 2))
        t = acc[pl.ds(pl.multiple_of(slot * BLK, BLK), BLK), b * NH + lo : b * NH + hi]
        return (t + RB[b, i, :, lo:hi].astype(jnp.float32)).astype(jnp.bfloat16)

    with jax.named_scope('p20_keepkv'):
        for i in range(4):
            ref = KV.at[2 * i + yh]
            ref[:, 0:HD] = total(i, 0, 512, NH)
            ref[:, HD:NKV] = total(i, 1, 512, NH)
            cp = pltpu.make_async_remote_copy(
                ref, ref, kvs, kvr.at[i], device_id=pair, device_id_type=MESH
            )
            cp.start()
    with jax.named_scope('p20_o'):
        o_over([(3, 0, (0,))], 0, 2)
        o_over([(3, 0, (2, 3)), (1, 0, (2, 3))], 2, 4)
    with jax.named_scope('p21_q'):
        add_up(1, 0, 4, 0, 512)
    with jax.named_scope('p21_rbq'):
        partial(RB, 0, 512).wait_recv()
    with jax.named_scope('p21_keepq'):
        for i in range(4):
            Q[i, :, 0:512] = total(i, 0, 0, 512)
            Q[i, :, 512:NQ] = total(i, 1, 0, 512)
    with jax.named_scope('p21_o'):
        o_over([(3, 0, (0,))], 2, 4, True)
        o_over([(0, 0, (2, 3))], 1, 2, True)
        o_over([(3, 0, (2, 3))], 0, 2, True)
        o_over([(1, 0, (2, 3))], 0, 2)
    scale = HD ** (-0.5)

    def h_ref(j, a, u):
        sg = 1 - 2 * a
        return HG.at[j, (x + 4 + sg * u) % 4, 2 * a : 2 * a + 2]

    def h_send(j, a, u, k):
        sg = 1 - 2 * a
        r = 1 if k != 1 else -1
        ref = h_ref(j, a, u)
        pltpu.make_async_remote_copy(
            ref, ref, hs.at[k], hr.at[j, a if (u - r) % 4 == 3 else 2],
            device_id=at_x(r * sg), device_id_type=MESH,
        ).start()

    def h_wait(ref, j, k):
        pltpu.make_async_remote_copy(
            ref, ref, hs.at[0], hr.at[j, k], device_id=sib, device_id_type=MESH
        ).wait_recv()

    def attend(j):
        rows = pl.ds(pl.multiple_of(j * 32, 32), 32)
        for i in range(4):
            nk = (2 * i + 2) * BLK
            if j == 0:
                ref = KV.at[2 * i + 1 - yh]
                pltpu.make_async_remote_copy(
                    ref, ref, kvs, kvr.at[i], device_id=pair, device_id_type=MESH
                ).wait_recv()
            q = jnp.concatenate(
                [Q[i, rows, h * HD : (h + 1) * HD] for h in range(8)], axis=0
            )
            kk = KV[0 : 2 * i + 2, :, 0:HD].reshape(nk, HD)
            vv = KV[0 : 2 * i + 2, :, HD:NKV].reshape(nk, HD)
            s = lax.dot_general(
                q, kk, (((1,), (1,)), ((), ())), preferred_element_type=jnp.float32
            ) * scale
            qpos = (2 * i + yh) * BLK + j * 32 + lax.broadcasted_iota(
                jnp.int32, (256, nk), 0
            ) % 32
            kpos = lax.broadcasted_iota(jnp.int32, (256, nk), 1)
            s = jnp.where(qpos >= kpos, s, jnp.float32(-1e30))
            e = jnp.exp(s - jnp.max(s, axis=-1, keepdims=True))
            pr = (e * (1.0 / jnp.sum(e, axis=-1, keepdims=True))).astype(jnp.bfloat16)
            o = jnp.dot(pr, vv, preferred_element_type=jnp.float32).astype(jnp.bfloat16)
            for h in range(8):
                HG[j, x, i, :, h * HD : (h + 1) * HD] = o[h * 32 : (h + 1) * 32]
            if i % 2:
                h_send(j, i // 2, 0, 0)
                h_send(j, i // 2, 0, 1)

    def h_forward(j):
        for a in (0, 1):
            h_wait(h_ref(j, a, 3), j, a)
            h_send(j, a, 3, 2)

    with jax.named_scope('p24_attend0'):
        attend(0)
    with jax.named_scope('p24_attend1'):
        attend(1)
    with jax.named_scope('p24_attend2'):
        attend(2)
    with jax.named_scope('p24a_o3'):
        o_over([(0, 3, (2,)), (2, 0, (2, 3)), (3, 3, (2,))], 2, 4)
    with jax.named_scope('p24d_hf0'):
        h_forward(0)
    with jax.named_scope('p24d_o4'):
        o_over([(2, 0, (2, 3)), (0, 3, (2,))], 0, 2)
        o_over([(1, 3, (2,))], 2, 4)
    with jax.named_scope('p24e_attend3'):
        attend(3)
    with jax.named_scope('p24e_o5'):
        o_over([(2, 3, (2,))], 2, 4)
    with jax.named_scope('p24f_hf1'):
        h_forward(1)
    with jax.named_scope('p24g_o6'):
        o_over([(3, 3, (2,)), (1, 3, (2,))], 0, 2)
    with jax.named_scope('p24g_hf2'):
        h_forward(2)
    with jax.named_scope('p24h_o7'):
        o_over([(2, 3, (2,))], 0, 2)
    with jax.named_scope('p25_o5'):
        o_wave(5)
    with jax.named_scope('p26_odone0'):
        o_arrived(0)

    def out_ref(j, xx):
        return out.at[
            pl.ds(pl.multiple_of(j * 32, 32), 32), pl.ds(pl.multiple_of(xx * NO, NO), NO)
        ]

    order = [(0, 0), (0, 1), (0, 3), (1, 0), (1, 1), (1, 3), (3, 0), (3, 1)]
    order += [(3, 3), (0, 2), (1, 2), (3, 2), (2, 0), (2, 1), (2, 2), (2, 3)]

    def chip_at(q):
        yy, zz = (y + order[q][0]) % 4, (z + order[q][1]) % 4
        return (yy // 2) * 8 + 2 * zz + yy % 2

    def tile(j, n):
        t = jnp.zeros((BLK, 512), jnp.float32)
        for kc in range(8):
            wo = jnp.concatenate(
                [WO[2 * chip_at(4 * n + e) + kc // 4, kc % 4] for e in range(4)], axis=1
            )
            lhs = HG[j, kc // 2, :, :, (kc % 2) * 512 : (kc % 2) * 512 + 512].reshape(BLK, 512)
            t += jnp.dot(lhs, wo, preferred_element_type=jnp.float32)
        OB[j, :, :, n * 512 : (n + 1) * 512] = t.astype(jnp.bfloat16).reshape(4, 32, 512)
        for q in range(4 * n, 4 * n + 4):
            col = pl.multiple_of(x * NO + chip_at(q) * BLK, BLK)
            dst = out.at[pl.ds(pl.multiple_of(j * 32, 32), 32), pl.ds(col, BLK)]
            cols = slice(q * BLK, (q + 1) * BLK)
            for r in (2, 1, 3):
                pltpu.make_async_remote_copy(
                    OB.at[j, (x + r) % 4, :, cols], dst, os_.at[r - 1], or_.at[3 - r],
                    device_id=at_x(r), device_id_type=MESH,
                ).start()
            pltpu.make_async_copy(OB.at[j, x, :, cols], dst, ol).start()

    def early(j, _):
        with jax.named_scope('m_wait'):
            h_wait(HG.at[j, 0:2], j, 2)
        tile(j, 0)
        tile(j, 1)
        return 0

    def late(j, _):
        tile(j, 2)
        tile(j, 3)
        return 0

    with jax.named_scope('p27_mix0'):
        lax.fori_loop(0, 1, early, 0)
    with jax.named_scope('p27_mix0_hf3'):
        h_forward(3)
    with jax.named_scope('p27_mix1'):
        lax.fori_loop(1, 2, early, 0)
    with jax.named_scope('p27_o6'):
        o_wave(6)
    with jax.named_scope('p27_p_mix2'):
        lax.fori_loop(2, 3, early, 0)
    with jax.named_scope('p27_q_odone1'):
        o_arrived(1)
    with jax.named_scope('p27_r_late'):
        lax.fori_loop(0, 2, late, 0)
    with jax.named_scope('p27_s_mix3'):
        lax.fori_loop(3, 4, early, 0)
    with jax.named_scope('p27_t_late'):
        lax.fori_loop(2, 4, late, 0)

    with jax.named_scope('p28_sent'):
        x_wait(X.at[:, 0:3], 0).wait_send()
        for n0, n1 in ((512, NH), (0, 512)):
            partial(PB, n0, n1).wait_send()
        d = KV.at[0:4]
        pltpu.make_async_remote_copy(
            d, d, kvs, kvr.at[0], device_id=pair, device_id_type=MESH
        ).wait_send()
        d = W.at[:, 0, :, 0, 0, 0, 0]
        pltpu.make_async_remote_copy(
            d, d, xs, xr.at[0], device_id=at_x(2), device_id_type=MESH
        ).wait_send()
        wo_swap.wait_send()
        r_sent()
        w_sent()
        o_sent()
        for k in range(3):
            pltpu.make_async_remote_copy(
                HG.at[0], HG.at[0], hs.at[k], hr.at[0, 0], device_id=sib, device_id_type=MESH
            ).wait_send()
    with jax.named_scope('p29_finish'):
        for r in (1, 2, 3):
            pltpu.make_async_remote_copy(
                OB.at[0], OB.at[0], os_.at[r - 1], or_.at[r - 1],
                device_id=sib, device_id_type=MESH,
            ).wait()
        pltpu.make_async_copy(OB.at[0], OB.at[0], ol).wait()


def add_rows(tok, branch, out, a, b, o, ins, outs):
    loads = [
        [
            pltpu.make_async_copy(src.at[16 * k : 16 * k + 16], dst.at[k], ins.at[t, k])
            for t, (src, dst) in enumerate(((branch, b), (tok, a)))
        ]
        for k in range(8)
    ]
    for pair in loads:
        for cp in pair:
            cp.start()
    stores = []
    for k in range(8):
        for cp in loads[k]:
            cp.wait()
        o[k] = a[k].astype(jnp.float32) + b[k].astype(jnp.float32)
        stores.append(pltpu.make_async_copy(o.at[k], out.at[16 * k : 16 * k + 16], outs.at[k]))
        stores[-1].start()
    for cp in stores:
        cp.wait()


def body(tokens, norm_gain, w_query, key_weight, value_weight, w_out):
    hbm = pl.BlockSpec(memory_space=pltpu.HBM)
    vmem = pl.BlockSpec(memory_space=pltpu.VMEM)
    bf = jnp.bfloat16
    dma = pltpu.SemaphoreType.DMA
    branch = pl.pallas_call(
        kernel,
        out_shape=jax.ShapeDtypeStruct((BLK, D), bf),
        in_specs=[hbm, vmem, hbm, hbm, hbm, hbm],
        out_specs=hbm,
        scratch_shapes=[
            pltpu.VMEM((2, 2, 2, 2, 4, 2, 2, 64, NH), bf),
            pltpu.VMEM((32, 4, 512, BLK), bf),
            pltpu.VMEM((BLK, D), bf),
            pltpu.VMEM((2, 4, BLK, 2048), bf),
            pltpu.VMEM((4, BLK, NQ), bf),
            pltpu.VMEM((8, BLK, NKV), bf),
            pltpu.VMEM((4, 4, 4, 32, NQ), bf),
            pltpu.VMEM((4, 4, 32, NO), bf),
            pltpu.VMEM((4 * BLK, NW), jnp.float32),
            pltpu.VMEM((2, 64, 2048), bf),
            pltpu.VMEM((4, 2, BLK, NH), bf),
            pltpu.VMEM((2, 4, BLK, NH), bf),
            dma((6,)), dma(()), dma((2,)), dma(()), dma((2,)), dma((2,)), dma((2,)),
            dma((2, 5)), dma((2, 4, 9)), dma((2, 2)),
            dma((5,)), dma((4, 9)), dma((2,)),
            dma(()), dma((4,)), dma((3,)), dma((4, 3)),
            dma((3,)), dma((3,)), dma(()),
        ],
        compiler_params=pltpu.CompilerParams(
            collective_id=0, has_side_effects=True, vmem_limit_bytes=60600000
        ),
        name="sublayer",
    )(tokens[0], norm_gain.reshape(1, D), w_query, key_weight, value_weight, w_out.T)
    total = pl.pallas_call(
        add_rows,
        out_shape=jax.ShapeDtypeStruct((BLK, D), jnp.float32),
        in_specs=[hbm, hbm],
        out_specs=hbm,
        scratch_shapes=[
            pltpu.VMEM((8, 16, D), bf),
            pltpu.VMEM((8, 16, D), bf),
            pltpu.VMEM((8, 16, D), jnp.float32),
            dma((2, 8)),
            dma((8,)),
        ],
        compiler_params=pltpu.CompilerParams(vmem_limit_bytes=64400000),
        name="add_rows",
    )(tokens[0], branch)
    return total[None]


def solution(mesh):
    placed = (
        P("fsdp", "seq", None),
        P(),
        P(("seq", "fsdp"), None),
        P(("seq", "fsdp"), None),
        P(("seq", "fsdp"), None),
        P(None, ("seq", "fsdp")),
    )
    return jax.shard_map(
        body, mesh=mesh, in_specs=placed, out_specs=P("fsdp", "seq", None), check_vma=False
    )
```
